32 devices in a mesh: dp: 8 (over y, x, core), tensor: 4 (over z).
Axes of the slice: x: 2, y: 2, z: 4, core: 2. Of those that a mesh axis runs over, the one named last changes fastest.
Arguments:
- tokens: bfloat16 [32768, 768], P(('dp', 'tensor')), may hold values from -6 to 6
- cotangent: bfloat16 [32768, 768], P(('dp', 'tensor')), may hold values from -6 to 6
- lengths: int32 [32, 6], P('dp'), may hold values from 1 to 256, 1024 in all within a row
- drop_mask: int32 [2, 2, 32, 6], P(None, None, 'dp'), may hold values 0 or 1
- ln1_gain: float32 [2, 768], replicated, may hold values from 0.5 to 1.5
- ln1_bias: float32 [2, 768], replicated, may hold values from -1.25 to 1.25
- w_qkv: bfloat16 [2, 768, 3, 768], P(None, None, None, 'tensor'), may hold values from -0.21875 to 0.21875
- b_qv: bfloat16 [2, 2, 768], P(None, None, 'tensor'), may hold values from -1.75 to 1.75
- w_out: bfloat16 [2, 768, 768], P(None, 'tensor'), may hold values from -0.875 to 0.875
- b_out: bfloat16 [2, 768], replicated, may hold values from -1.75 to 1.75
- ln2_gain: float32 [2, 768], replicated, may hold values from 0.5 to 1.5
- ln2_bias: float32 [2, 768], replicated, may hold values from -1.25 to 1.25
- w_up: bfloat16 [2, 768, 3072], P(None, None, 'tensor'), may hold values from -0.21875 to 0.21875
- b_up: bfloat16 [2, 3072], P(None, 'tensor'), may hold values from -1.75 to 1.75
- w_down: bfloat16 [2, 3072, 768], P(None, 'tensor'), may hold values from -0.109375 to 0.109375
- b_down: bfloat16 [2, 768], replicated, may hold values from -1.75 to 1.75
Outputs:
- blocks_out: bfloat16 [2, 32768, 768], P(None, ('dp', 'tensor'))
- input_grad: float32 [32768, 768], P(('dp', 'tensor'))
- ln1_gain_grad: float32 [2, 768], replicated
- ln1_bias_grad: float32 [2, 768], replicated
- w_qkv_grad: float32 [2, 768, 3, 768], P(None, 'dp', None, 'tensor')
- b_qv_grad: float32 [2, 2, 768], replicated
- w_out_grad: float32 [2, 768, 768], P(None, 'tensor', 'dp')
- b_out_grad: float32 [2, 768], replicated
- ln2_gain_grad: float32 [2, 768], replicated
- ln2_bias_grad: float32 [2, 768], replicated
- w_up_grad: float32 [2, 768, 3072], P(None, 'dp', 'tensor')
- b_up_grad: float32 [2, 3072], replicated
- w_down_grad: float32 [2, 3072, 768], P(None, 'tensor', 'dp')
- b_down_grad: float32 [2, 768], replicated
The draws below stay inside these ranges and needn't reach their ends.
Inputs may be any that keep to these rules, and one draw needn't show every extreme that they name: Each row's 6 lengths sum to 1024, and the largest in each row is 256.
All inputs are finite; a program needn't handle non-finite values. No bound on the sum of `drop_mask` on one device may be relied on, other than what follows from the above.
Results may differ from the reference program's by a relative error of at most 0.02.
Values may be sent and summed in bfloat16 or wider, within the bound.
A program may use at most 320 MiB of HBM per device.

```python
import math
import jax
import jax.numpy as jnp
import numpy as np
from jax import lax

D = 768
HEADS = 12
HEAD_DIM = 64
FF = 3072
LAYERS = 2
SEQ = 1024
SEGS = 6
MOST_LEN = 256
ROWS_DEV = 4
ROWS = 32
TOKENS = 32768
N_DP = 8


def place_ends(drawn, stream_key, low, largest):
    longest = drawn.shape.index(max(drawn.shape))
    spots = []
    for shift in (0, 1):
        where = [jax.random.randint(jax.random.fold_in(stream_key, axis), (), 0, length) for axis, length in enumerate(drawn.shape)]
        where[longest] = (where[longest] + shift) % drawn.shape[longest]
        spots.append(tuple(where))
    return drawn.at[spots[0]].set(low).at[spots[1]].set(largest)


def strengthened(values, stream_key, source, target, shards_of, factor):
    def block_of(position):
        return (jnp.arange(values.shape[position]) // (values.shape[position] // shards_of)).reshape((-1,) + (1,) * (values.ndim - 1 - position))

    one_side = jax.random.permutation(stream_key, shards_of)[block_of(target)]
    second = (block_of(target) + shards_of // 2) % shards_of
    return jnp.where((block_of(source) == one_side) | (block_of(source) == second), factor * values, values)


def level_of(key, shape, cuts, least, top_value):
    gain = 1.0
    for dim, shards_of in cuts:
        draws = jax.random.uniform(jax.random.fold_in(jax.random.fold_in(key, 6), dim), (shards_of,), jnp.float32, least / len(cuts), top_value / len(cuts))
        gain = gain * jnp.repeat(jnp.exp(draws), shape[dim] // shards_of).reshape((-1,) + (1,) * (len(shape) - 1 - dim))
    return gain


def length_profile(amount, total, reach, skew):
    weights = [(1 << 20) // math.isqrt(standing ** skew) + 1 for standing in range(2, amount + 1)]
    surplus, counts = total - reach - (amount - 1), [1] * (amount - 1)
    while surplus > 0:
        free = [i for i in range(amount - 1) if counts[i] < reach]
        mass, remaining = sum([weights[i] for i in free]), surplus
        for i in free:
            addition = min(reach - counts[i], max(1, remaining * weights[i] // mass), surplus)
            counts[i] = counts[i] + addition
            surplus = surplus - addition
    return np.array([reach] + counts)


def ragged_sizes(stream_key, count, total, bound, slope):
    if count == 2:
        one = jax.random.randint(stream_key, (), max(1, total - bound), min(bound, total - 1) + 1)
        return jnp.stack([one, total - one])
    tallies = jnp.asarray(length_profile(count, total, bound, slope), jnp.int32)
    twos = (count - 1) // 2
    donor, receiver = tallies[1:1 + 2 * twos:2], tallies[2:2 + 2 * twos:2]
    room = jnp.minimum(donor - 1, bound - receiver)
    shifted = jax.random.randint(jax.random.fold_in(stream_key, 1), (twos,), 0, 1 << 20) % (room + 1)
    tallies = tallies.at[1:1 + 2 * twos:2].set(donor - shifted).at[2:2 + 2 * twos:2].set(receiver + shifted)
    return tallies[jax.random.permutation(jax.random.fold_in(stream_key, 2), count)]


def normal_values(stream_key, dims, width, reach, split=(), kind=jnp.bfloat16):
    level = level_of(stream_key, dims, split, -0.22, 0.18) if split else 1.0
    values = jax.random.normal(stream_key, dims, jnp.float32) * width * level
    return jnp.minimum(jnp.maximum(values, -reach), reach).astype(kind)


def heavy_noise(own_key, shape, width, limit, pieces, heavy, kind=jnp.bfloat16):
    entries = width * jax.random.normal(own_key, shape, jnp.float32)
    if pieces:
        entries = entries * level_of(own_key, shape, pieces, -0.22, 0.18)
    return jnp.clip(strengthened(entries, jax.random.fold_in(own_key, 3), *heavy), -limit, limit).astype(kind)


def setup_inputs(seed: int = 0) -> dict:
    key_of = jax.random.split(jax.random.key(seed), 17)
    return {
        "tokens": heavy_noise(key_of[0], (TOKENS, D), 1.0, 6.0, ((0, 32),), (0, 1, 32, 2.75)),
        "cotangent": heavy_noise(key_of[1], (TOKENS, D), 1.0, 6.0, ((0, 32),), (0, 1, 32, 2.75)),
        "lengths": jax.vmap(lambda own: ragged_sizes(own, SEGS, SEQ, MOST_LEN, 2))(jax.random.split(key_of[2], ROWS)).reshape((ROWS, SEGS)).astype(jnp.int32),
        "drop_mask": place_ends((jax.random.randint(key_of[3], (LAYERS, 2, ROWS, SEGS), 0, 10) < 9).astype(jnp.int32), jax.random.fold_in(key_of[3], 1), 0, 1),
        "ln1_gain": jnp.clip(1.0 + 0.1 * jax.random.normal(key_of[4], (LAYERS, D), jnp.float32), 0.5, 1.5),
        "ln1_bias": normal_values(key_of[5], (LAYERS, D), 0.2, 1.25, (), jnp.float32),
        "w_qkv": normal_values(key_of[6], (LAYERS, D, 3, D), D ** -0.5, 0.21875, ((3, 4),)),
        "b_qv": normal_values(key_of[7], (LAYERS, 2, D), 0.3, 1.75, ((2, 4),)),
        "w_out": normal_values(key_of[8], (LAYERS, D, D), (D // 16) ** -0.5, 0.875, ((1, 4),)),
        "b_out": normal_values(key_of[9], (LAYERS, D), 0.3, 1.75),
        "ln2_gain": jnp.clip(1.0 + 0.1 * jax.random.normal(key_of[10], (LAYERS, D), jnp.float32), 0.5, 1.5),
        "ln2_bias": normal_values(key_of[11], (LAYERS, D), 0.2, 1.25, (), jnp.float32),
        "w_up": normal_values(key_of[12], (LAYERS, D, FF), D ** -0.5, 0.21875, ((2, 4),)),
        "b_up": normal_values(key_of[13], (LAYERS, FF), 0.3, 1.75, ((1, 4),)),
        "w_down": normal_values(key_of[14], (LAYERS, FF, D), FF ** -0.5, 0.109375, ((1, 4),)),
        "b_down": normal_values(key_of[15], (LAYERS, D), 0.3, 1.75),
    }


@jax.custom_vjp
def low(v):
    return lax.optimization_barrier(v.astype(jnp.bfloat16)).astype(jnp.float32)

@jax.custom_vjp
def low_back(v):
    return v

def low_keep(v):
    return (low(v), None)

def low_pass(kept, grad):
    return (grad,)

def back_keep(v):
    return (v, None)

def back_low(kept, grad):
    return (low(grad),)
low.defvjp(low_keep, low_pass)
low_back.defvjp(back_keep, back_low)
eps_norm = 1e-06
survival = 0.9
masked_score = -1e+30
highest = lax.Precision.HIGHEST

def layer_norm(values, norm_gain, norm_shift):
    centre = values - lax.optimization_barrier(jnp.mean(values, axis=-1, keepdims=True))
    spread = lax.optimization_barrier(jnp.mean(centre * centre, axis=-1, keepdims=True))
    return centre * lax.rsqrt(spread + eps_norm) * norm_gain + norm_shift

def matmul(left_side, right_side):
    return jnp.dot(left_side, right_side, precision=highest)

def attend_row(query_row, key_row, value_row, segment_row):
    scores = jnp.einsum('qhd,khd->hqk', query_row, key_row, precision=highest) * (1.0 / math.sqrt(HEAD_DIM))
    scores = low_back(scores)
    same_segment = (segment_row[:, None] == segment_row[None, :])[None]
    scores = jnp.where(same_segment, scores, masked_score)
    row_top = lax.optimization_barrier(jnp.max(scores, axis=-1, keepdims=True))
    exponent = jnp.exp(scores - row_top)
    weights_soft = low(exponent / lax.optimization_barrier(jnp.sum(exponent, axis=-1, keepdims=True)))
    return jnp.einsum('hqk,khd->qhd', weights_soft, value_row, precision=highest)
checked_row = jax.checkpoint(attend_row)

def forward(group_in, weights, group_keep, group_segments):
    row_number = group_segments.shape[0]
    hidden = group_in
    produced = []
    for layer_index in range(LAYERS):
        gain_one, shift_one, weight_qkv, bias_qv, weight_out, bias_out, gain_two, shift_two, weight_up, bias_up, weight_down, bias_down = [entry[layer_index] for entry in weights]
        normed_one = low(layer_norm(hidden, gain_one, shift_one))
        project = low_back(matmul(normed_one, weight_qkv.reshape(D, 3 * D))).reshape(-1, 3, D)
        queries = low(project[:, 0] + bias_qv[0]).reshape(row_number, SEQ, HEADS, HEAD_DIM)
        keys_all = low(project[:, 1]).reshape(row_number, SEQ, HEADS, HEAD_DIM)
        values_all = low(project[:, 2] + bias_qv[1]).reshape(row_number, SEQ, HEADS, HEAD_DIM)
        mixed_out = lax.map(lambda row_item: checked_row(*row_item), (queries, keys_all, values_all, group_segments))
        mixed_low = low_back(low(mixed_out.reshape(-1, D)))
        middle = hidden + group_keep[layer_index, 0][:, None] * (low_back(matmul(mixed_low, weight_out)) + bias_out)
        normed_two = low(layer_norm(middle, gain_two, shift_two))
        upward = low_back(matmul(normed_two, weight_up)) + bias_up
        active = low(jax.nn.gelu(upward, approximate=False))
        hidden = middle + group_keep[layer_index, 1][:, None] * (low_back(matmul(active, weight_down)) + bias_down)
        produced.append(hidden)
    return jnp.stack(produced)

def reference(tokens, cotangent, lengths, drop_mask, ln1_gain, ln1_bias, w_qkv, b_qv, w_out, b_out, ln2_gain, ln2_bias, w_up, b_up, w_down, b_down):
    weights = tuple((entry.astype(jnp.float32) for entry in (ln1_gain, ln1_bias, w_qkv, b_qv, w_out, b_out, ln2_gain, ln2_bias, w_up, b_up, w_down, b_down)))
    segment_ends = jnp.cumsum(lengths, axis=-1).astype(jnp.int32)
    positions = jnp.arange(SEQ, dtype=jnp.int32)
    segments = lax.optimization_barrier(jnp.sum((positions[None, :, None] >= segment_ends[:, None, :]).astype(jnp.int32), axis=-1)).astype(jnp.int32)
    onehot = (segments[:, :, None] == jnp.arange(SEGS, dtype=jnp.int32)[None, None, :]).astype(jnp.float32)
    keep_rows = lax.optimization_barrier(jnp.sum(onehot[None, None] * drop_mask.astype(jnp.float32)[:, :, :, None, :], axis=-1)) / survival
    group_tokens = ROWS_DEV * SEQ
    keep_groups = keep_rows.reshape(LAYERS, 2, N_DP, group_tokens).transpose(2, 0, 1, 3)
    segment_groups = segments.reshape(N_DP, ROWS_DEV, SEQ)
    input_groups = tokens.astype(jnp.float32).reshape(N_DP, group_tokens, D)
    seed_groups = cotangent.astype(jnp.float32).reshape(N_DP, group_tokens, D)

    def group_step(totals, group_item):
        group_in, group_seed, group_keep, group_segments = group_item

        def run_layers(values, params):
            return forward(values, params, group_keep, group_segments)
        produced, pullback = jax.vjp(run_layers, group_in, weights)
        seed_out = jnp.concatenate([jnp.zeros_like(produced[:-1]), group_seed[None]], axis=0)
        grad_in, grad_weights = pullback(seed_out)
        return (tuple((total + grad_part for total, grad_part in zip(totals, grad_weights))), (produced, grad_in))
    zero_totals = tuple((jnp.zeros(entry.shape, jnp.float32) for entry in weights))
    totals, (produced, grad_in) = lax.scan(group_step, zero_totals, (input_groups, seed_groups, keep_groups, segment_groups))
    blocks_out = produced.transpose(1, 0, 2, 3).reshape(LAYERS, N_DP * group_tokens, D).astype(jnp.bfloat16)
    input_grad = grad_in.reshape(N_DP * group_tokens, D)
    return (blocks_out, input_grad, totals[0], totals[1], totals[2], totals[3], totals[4], totals[5], totals[6], totals[7], totals[8], totals[9], totals[10], totals[11])
```

```python
import math

import jax
import jax.numpy as jnp
from jax import lax
from jax.experimental import pallas as pl
from jax.experimental.pallas import tpu as pltpu
from jax.sharding import PartitionSpec as P

HEAD_DIM = 64
SEQ = 1024
MOST_LEN = 256
PAIR = 2 * HEAD_DIM

eps_norm = 1e-06
survival = 0.9
masked_score = -1e30
score_scale = 1.0 / math.sqrt(HEAD_DIM)
groups = ("dp", "tensor")
bf16 = jnp.bfloat16
f32 = jnp.float32


def norm_forward(values, norm_gain, norm_shift):
    centre = values - jnp.mean(values, axis=-1, keepdims=True)
    spread = jnp.mean(centre * centre, axis=-1, keepdims=True)
    scaled = lax.rsqrt(spread + eps_norm)
    normalized = centre * scaled
    return (normalized * norm_gain + norm_shift, normalized, scaled)


def norm_backward(grad_out, normalized, scaled, norm_gain):
    grad_unit = grad_out * norm_gain
    inner = (
        grad_unit
        - jnp.mean(grad_unit, axis=-1, keepdims=True)
        - normalized * jnp.mean(grad_unit * normalized, axis=-1, keepdims=True)
    )
    return (inner * scaled, jnp.sum(grad_out * normalized, axis=0), jnp.sum(grad_out, axis=0))


def key_window(block):
    return max(0, (block - 1) * MOST_LEN), min(SEQ, (block + 2) * MOST_LEN)


def own_lanes(head):
    lane = lax.broadcasted_iota(jnp.int32, (1, PAIR), 1)
    return lane < HEAD_DIM if head == 0 else lane >= HEAD_DIM


def dot_rows(left, right):
    return lax.dot_general(left, right, (((1,), (1,)), ((), ())), preferred_element_type=f32)


def dot_tokens(left, right):
    return lax.dot_general(left, right, (((0,), (0,)), ((), ())), preferred_element_type=f32)


def attention_forward_kernel(q_ref, k_ref, v_ref, fq_ref, fk_ref, mixed_ref, total_ref):
    for block in range(SEQ // MOST_LEN):
        rows = slice(block * MOST_LEN, (block + 1) * MOST_LEN)
        keys = slice(*key_window(block))
        mixed = []
        totals = []
        for head in (0, 1):
            own = own_lanes(head)
            query = jnp.where(own, q_ref[rows, :] * bf16(score_scale), fq_ref[rows, :])
            key = jnp.where(own, k_ref[keys, :], fk_ref[keys, :])
            scores = dot_rows(query, key)
            top = jnp.max(scores, axis=-1, keepdims=True)
            exponent = jnp.exp(scores - top)
            total = jnp.sum(exponent, axis=-1, keepdims=True)
            part = jnp.dot(exponent.astype(bf16), v_ref[keys, :], preferred_element_type=f32)
            mixed.append(part / total)
            totals.append(top + jnp.log(total))
        own = own_lanes(0)
        mixed_ref[rows, :] = jnp.where(own, mixed[0], mixed[1]).astype(bf16)
        total_ref[rows, :] = jnp.where(own, totals[0], totals[1])


def attention_backward_kernel(
    q_ref, k_ref, v_ref, fq_ref, fk_ref, grad_ref, total_ref,
    dq_ref, dk_ref, dv_ref, sums_ref, dk_acc, dv_acc,
):
    dk_acc[...] = jnp.zeros_like(dk_acc)
    dv_acc[...] = jnp.zeros_like(dv_acc)
    query_sum = jnp.zeros((1, PAIR), f32)
    for block in range(SEQ // MOST_LEN):
        rows = slice(block * MOST_LEN, (block + 1) * MOST_LEN)
        keys = slice(*key_window(block))
        grad_query = jnp.zeros((MOST_LEN, PAIR), f32)
        for head in (0, 1):
            own = own_lanes(head)
            scaled = q_ref[rows, :] * bf16(score_scale)
            query = jnp.where(own, scaled, fq_ref[rows, :])
            key = jnp.where(own, k_ref[keys, :], fk_ref[keys, :])
            scores = dot_rows(query, key)
            lane = head * HEAD_DIM
            weights = jnp.exp(scores - total_ref[rows, lane : lane + 1])
            zero = jnp.zeros((), bf16)
            grad = jnp.where(own, grad_ref[rows, :], zero)
            product = weights * dot_rows(grad, v_ref[keys, :])
            inner = jnp.sum(product, axis=-1, keepdims=True)
            grad_scores = (product - weights * inner).astype(bf16)
            grad_query += jnp.dot(
                grad_scores, jnp.where(own, k_ref[keys, :], zero), preferred_element_type=f32
            )
            dk_acc[keys, :] += dot_tokens(grad_scores, jnp.where(own, scaled, zero))
            dv_acc[keys, :] += dot_tokens(weights.astype(bf16), grad)
        grad_query *= score_scale
        query_sum += jnp.sum(grad_query, axis=0, keepdims=True)
        dq_ref[rows, :] = grad_query.astype(bf16)
    dk_ref[...] = dk_acc[...].astype(bf16)
    dv_ref[...] = dv_acc[...].astype(bf16)
    value_sum = jnp.sum(dv_acc[...], axis=0, keepdims=True)
    row = lax.broadcasted_iota(jnp.int32, (8, PAIR), 0)
    sums_ref[0, :, :] = jnp.where(row == 0, query_sum, value_sum)


def attention_specs(pairs):
    def part(index):
        return pl.BlockSpec((SEQ, PAIR), lambda r, p: (r, index * pairs + p))

    feature = pl.BlockSpec((SEQ, PAIR), lambda r, p: (r, 0))
    own = pl.BlockSpec((SEQ, PAIR), lambda r, p: (r, p))
    return [part(0), part(1), part(2), feature, feature], own


def attention_forward(project, feature_q, feature_k):
    tokens, width = project.shape[0], project.shape[1] // 3
    pairs = width // PAIR
    ins, own = attention_specs(pairs)
    return pl.pallas_call(
        attention_forward_kernel,
        grid=(tokens // SEQ, pairs),
        in_specs=ins,
        out_specs=[own, own],
        out_shape=[
            jax.ShapeDtypeStruct((tokens, width), bf16),
            jax.ShapeDtypeStruct((tokens, width), f32),
        ],
        cost_estimate=pl.CostEstimate(
            flops=4 * tokens * 3 * MOST_LEN * 2 * width,
            bytes_accessed=tokens * width * 12,
            transcendentals=tokens * 3 * MOST_LEN * width // HEAD_DIM,
        ),
        compiler_params=pltpu.CompilerParams(vmem_limit_bytes=48 << 20),
        name="attend",
    )(project, project, project, feature_q, feature_k)


def attention_backward(project, feature_q, feature_k, grad_mixed, totals):
    tokens, width = grad_mixed.shape
    pairs = width // PAIR
    ins, own = attention_specs(pairs)
    low = jax.ShapeDtypeStruct((tokens, width), bf16)
    return pl.pallas_call(
        attention_backward_kernel,
        grid=(tokens // SEQ, pairs),
        in_specs=ins + [own, own],
        out_specs=[own, own, own, pl.BlockSpec((1, 8, PAIR), lambda r, p: (r, 0, p))],
        out_shape=[low, low, low, jax.ShapeDtypeStruct((tokens // SEQ, 8, width), f32)],
        scratch_shapes=[pltpu.VMEM((SEQ, PAIR), f32), pltpu.VMEM((SEQ, PAIR), f32)],
        cost_estimate=pl.CostEstimate(
            flops=10 * tokens * 3 * MOST_LEN * 2 * width,
            bytes_accessed=tokens * width * 18,
            transcendentals=tokens * 3 * MOST_LEN * width // HEAD_DIM,
        ),
        compiler_params=pltpu.CompilerParams(vmem_limit_bytes=48 << 20),
        name="attend_back",
    )(project, project, project, feature_q, feature_k, grad_mixed, totals)


def per_device(
    tokens,
    cotangent,
    lengths,
    drop_mask,
    ln1_gain,
    ln1_bias,
    w_qkv,
    b_qv,
    w_out,
    b_out,
    ln2_gain,
    ln2_bias,
    w_up,
    b_up,
    w_down,
    b_down,
):
    layer_count = w_qkv.shape[0]
    local_rows, width = tokens.shape
    segment_count = lengths.shape[1]
    tensor_index = lax.axis_index("tensor")
    dp_index = lax.axis_index("dp")
    n_dp = lax.axis_size("dp")
    n_tensor = lax.axis_size("tensor")
    own_rows = local_rows // SEQ
    head_cols = w_qkv.shape[3]
    hidden_cols = w_up.shape[2]
    piece = width // n_dp
    out_piece = head_cols // n_dp
    hidden_piece = hidden_cols // n_dp

    own_lengths = lax.dynamic_slice_in_dim(lengths, tensor_index * own_rows, own_rows, 0)
    own_mask = lax.dynamic_slice_in_dim(drop_mask, tensor_index * own_rows, own_rows, 2)
    segment_ends = jnp.cumsum(own_lengths, axis=-1)
    positions = jnp.arange(SEQ, dtype=jnp.int32)
    segments = jnp.sum(
        (positions[None, :, None] >= segment_ends[:, None, :]).astype(jnp.int32), axis=-1
    )
    onehot = (
        segments[:, :, None] == jnp.arange(segment_count, dtype=jnp.int32)[None, None, :]
    ).astype(f32)
    keep = (
        jnp.sum(onehot[None, None] * own_mask.astype(f32)[:, :, :, None, :], axis=-1) / survival
    ).reshape(layer_count, 2, local_rows)
    lane = jnp.arange(PAIR, dtype=jnp.int32)[None, :] % HEAD_DIM
    same = segments.reshape(local_rows, 1) == lane
    feature_q = same.astype(bf16)
    feature_k = jnp.where(same | (lane >= segment_count), 0.0, masked_score).astype(bf16)

    def gather(piece_in):
        gathered = lax.all_gather(piece_in, groups, axis=0, tiled=False)
        return gathered.reshape((n_dp, n_tensor) + piece_in.shape)

    def part_of(array, size, axis):
        return lax.dynamic_slice_in_dim(array, dp_index * size, size, axis)

    full_qkv, full_out, full_up, full_down = [], [], [], []
    for layer in range(layer_count):
        got = gather(part_of(w_qkv[layer], piece, 0).reshape(piece, 3 * head_cols))
        got = got.reshape(n_dp, n_tensor, piece, 3, head_cols).transpose(0, 2, 3, 1, 4)
        full_qkv.append(got.reshape(width, 3 * n_tensor * head_cols))
        rest = jnp.concatenate(
            [
                part_of(w_up[layer], piece, 0),
                part_of(w_down[layer], hidden_piece, 0),
                part_of(w_out[layer], out_piece, 0),
            ],
            axis=0,
        )
        got = gather(rest)
        full_up.append(
            got[:, :, :piece].transpose(0, 2, 1, 3).reshape(width, n_tensor * hidden_cols)
        )
        full_down.append(
            got[:, :, piece : piece + hidden_piece]
            .transpose(1, 0, 2, 3)
            .reshape(n_tensor * hidden_cols, width)
        )
        full_out.append(
            got[:, :, piece + hidden_piece :]
            .transpose(1, 0, 2, 3)
            .reshape(n_tensor * head_cols, width)
        )
    all_bias = lax.all_gather(
        jnp.concatenate([b_qv.reshape(-1), b_up.reshape(-1)]), "tensor", axis=0, tiled=False
    ).astype(f32)
    qv_count = layer_count * 2 * head_cols
    bias_qv = (
        all_bias[:, :qv_count]
        .reshape(n_tensor, layer_count, 2, head_cols)
        .transpose(1, 2, 0, 3)
        .reshape(layer_count, 2, width)
    )
    bias_up = (
        all_bias[:, qv_count:]
        .reshape(n_tensor, layer_count, hidden_cols)
        .transpose(1, 0, 2)
        .reshape(layer_count, n_tensor * hidden_cols)
    )

    hidden = tokens.astype(f32)
    produced = []
    kept = []
    for layer in range(layer_count):
        normed_one, unit_one, scaled_one = norm_forward(hidden, ln1_gain[layer], ln1_bias[layer])
        normed_one = normed_one.astype(bf16)
        bias = jnp.concatenate([bias_qv[layer, 0], jnp.zeros((width,), f32), bias_qv[layer, 1]])
        project = (
            jnp.dot(normed_one, full_qkv[layer], preferred_element_type=f32) + bias
        ).astype(bf16)
        mixed, totals = attention_forward(project, feature_q, feature_k)
        attn = jnp.dot(mixed, full_out[layer], preferred_element_type=f32)
        middle = hidden + keep[layer, 0][:, None] * (attn + b_out[layer].astype(f32))
        normed_two, unit_two, scaled_two = norm_forward(middle, ln2_gain[layer], ln2_bias[layer])
        normed_two = normed_two.astype(bf16)
        upward = jnp.dot(normed_two, full_up[layer], preferred_element_type=f32) + bias_up[layer]
        phi = 0.5 * (1.0 + lax.erf(upward * math.sqrt(0.5)))
        active = (upward * phi).astype(bf16)
        slope = phi + upward * (jnp.exp(-0.5 * upward * upward) * (1.0 / math.sqrt(2 * math.pi)))
        down = jnp.dot(active, full_down[layer], preferred_element_type=f32)
        hidden = middle + keep[layer, 1][:, None] * (down + b_down[layer].astype(f32))
        produced.append(hidden.astype(bf16))
        kept.append(
            (unit_one, scaled_one, normed_one, project, totals, mixed,
             unit_two, scaled_two, normed_two, active, slope)
        )
    blocks_out = jnp.stack(produced)

    def by_block(grad, columns):
        return (
            grad.astype(bf16)
            .reshape(n_dp, piece, n_tensor, columns)
            .transpose(0, 2, 1, 3)
        )

    def scatter(blocks):
        flat = blocks.reshape((n_dp * n_tensor * blocks.shape[2],) + blocks.shape[3:])
        return lax.psum_scatter(flat, groups, scatter_dimension=0, tiled=True).astype(f32)

    grad_flow = cotangent.astype(f32)
    collected = [None] * layer_count
    for layer in reversed(range(layer_count)):
        (unit_one, scaled_one, normed_one, project, totals, mixed,
         unit_two, scaled_two, normed_two, active, slope) = kept[layer]
        branch_two = keep[layer, 1][:, None] * grad_flow
        grad_bias_down = jnp.sum(branch_two, axis=0)
        branch_two = branch_two.astype(bf16)
        grad_down = by_block(dot_tokens(branch_two, active), hidden_cols)
        grad_up = dot_rows(branch_two, full_down[layer]) * slope
        grad_bias_up = jnp.sum(grad_up, axis=0)
        grad_up = grad_up.astype(bf16)
        grad_w_up = by_block(dot_tokens(normed_two, grad_up), hidden_cols)
        wide = scatter(jnp.concatenate([grad_w_up, grad_down], axis=2))
        grad_part, grad_gain_two, grad_shift_two = norm_backward(
            dot_rows(grad_up, full_up[layer]), unit_two, scaled_two, ln2_gain[layer]
        )
        grad_middle = grad_flow + grad_part
        branch_one = keep[layer, 0][:, None] * grad_middle
        grad_bias_out = jnp.sum(branch_one, axis=0)
        branch_one = branch_one.astype(bf16)
        grad_out = by_block(dot_tokens(branch_one, mixed), head_cols)
        grad_mixed = dot_rows(branch_one, full_out[layer]).astype(bf16)
        *grads, sums = attention_backward(project, feature_q, feature_k, grad_mixed, totals)
        grad_bias_qv = jnp.sum(sums, axis=0)[:2]
        weights = full_qkv[layer].reshape(width, 3, width)
        grad_one = sum(dot_rows(grads[part], weights[:, part]) for part in range(3))
        narrow = [by_block(dot_tokens(normed_one, grad), head_cols) for grad in grads]
        narrow = scatter(jnp.concatenate(narrow + [grad_out], axis=3))
        grad_part, grad_gain_one, grad_shift_one = norm_backward(
            grad_one, unit_one, scaled_one, ln1_gain[layer]
        )
        grad_flow = grad_middle + grad_part
        collected[layer] = (
            jnp.concatenate(
                [grad_gain_one, grad_shift_one, grad_bias_qv.reshape(-1), grad_bias_out,
                 grad_gain_two, grad_shift_two, grad_bias_down, grad_bias_up]
            ),
            narrow[:, : 3 * head_cols].reshape(piece, 3, head_cols),
            narrow[:, 3 * head_cols :].T,
            wide[:piece],
            wide[piece:].T,
        )
    small, grad_qkv, grad_out, grad_up, grad_down = [
        jnp.stack([entry[position] for entry in collected]) for position in range(5)
    ]
    small = lax.psum(small, groups)
    gain_one, shift_one, query_bias, value_bias, bias_out, gain_two, shift_two, bias_down = [
        small[:, position * width : (position + 1) * width] for position in range(8)
    ]
    return (
        blocks_out,
        grad_flow,
        gain_one,
        shift_one,
        grad_qkv,
        jnp.stack([query_bias, value_bias], axis=1),
        grad_out,
        bias_out,
        gain_two,
        shift_two,
        grad_up,
        small[:, 8 * width :],
        grad_down,
        bias_down,
    )


def solution(mesh):
    in_specs = (
        P(("dp", "tensor"), None),
        P(("dp", "tensor"), None),
        P("dp", None),
        P(None, None, "dp", None),
        P(),
        P(),
        P(None, None, None, "tensor"),
        P(None, None, "tensor"),
        P(None, "tensor", None),
        P(),
        P(),
        P(),
        P(None, None, "tensor"),
        P(None, "tensor"),
        P(None, "tensor", None),
        P(),
    )
    out_specs = (
        P(None, ("dp", "tensor"), None),
        P(("dp", "tensor"), None),
        P(),
        P(),
        P(None, "dp", None, "tensor"),
        P(),
        P(None, "tensor", "dp"),
        P(),
        P(),
        P(),
        P(None, "dp", "tensor"),
        P(),
        P(None, "tensor", "dp"),
        P(),
    )
    return jax.shard_map(
        per_device, mesh=mesh, in_specs=in_specs, out_specs=out_specs, check_vma=False
    )
```

```python
import math

import jax
import jax.numpy as jnp
from jax import lax
from jax.experimental import pallas as pl
from jax.experimental.pallas import tpu as pltpu
from jax.sharding import PartitionSpec as P

HEAD_DIM = 64
SEQ = 1024
MOST_LEN = 256
PAIR = 2 * HEAD_DIM

eps_norm = 1e-06
survival = 0.9
masked_score = -1e30
score_scale = 1.0 / math.sqrt(HEAD_DIM)
groups = ("dp", "tensor")
bf16 = jnp.bfloat16
f32 = jnp.float32


def norm_forward(values, norm_gain, norm_shift):
    centre = values - jnp.mean(values, axis=-1, keepdims=True)
    spread = jnp.mean(centre * centre, axis=-1, keepdims=True)
    scaled = lax.rsqrt(spread + eps_norm)
    normalized = centre * scaled
    return (normalized * norm_gain + norm_shift, normalized, scaled)


def norm_backward(grad_out, normalized, scaled, norm_gain):
    grad_unit = grad_out * norm_gain
    inner = (
        grad_unit
        - jnp.mean(grad_unit, axis=-1, keepdims=True)
        - normalized * jnp.mean(grad_unit * normalized, axis=-1, keepdims=True)
    )
    return (inner * scaled, jnp.sum(grad_out * normalized, axis=0), jnp.sum(grad_out, axis=0))


def key_window(block):
    return max(0, (block - 1) * MOST_LEN), min(SEQ, (block + 2) * MOST_LEN)


def own_lanes(head):
    lane = lax.broadcasted_iota(jnp.int32, (1, PAIR), 1)
    return lane < HEAD_DIM if head == 0 else lane >= HEAD_DIM


def dot_rows(left, right):
    return lax.dot_general(left, right, (((1,), (1,)), ((), ())), preferred_element_type=f32)


def dot_tokens(left, right):
    return lax.dot_general(left, right, (((0,), (0,)), ((), ())), preferred_element_type=f32)


def attention_forward_kernel(q_ref, k_ref, v_ref, fq_ref, fk_ref, mixed_ref, total_ref):
    for block in range(SEQ // MOST_LEN):
        rows = slice(block * MOST_LEN, (block + 1) * MOST_LEN)
        keys = slice(*key_window(block))
        mixed = []
        totals = []
        for head in (0, 1):
            own = own_lanes(head)
            query = jnp.where(own, q_ref[rows, :] * bf16(score_scale), fq_ref[rows, :])
            key = jnp.where(own, k_ref[keys, :], fk_ref[keys, :])
            scores = dot_rows(query, key)
            top = jnp.max(scores, axis=-1, keepdims=True)
            exponent = jnp.exp(scores - top)
            total = jnp.sum(exponent, axis=-1, keepdims=True)
            part = jnp.dot(exponent.astype(bf16), v_ref[keys, :], preferred_element_type=f32)
            mixed.append(part / total)
            totals.append(top + jnp.log(total))
        own = own_lanes(0)
        mixed_ref[rows, :] = jnp.where(own, mixed[0], mixed[1]).astype(bf16)
        total_ref[rows, :] = jnp.where(own, totals[0], totals[1])


def attention_backward_kernel(
    q_ref, k_ref, v_ref, fq_ref, fk_ref, grad_ref, total_ref,
    dq_ref, dk_ref, dv_ref, sums_ref, dk_acc, dv_acc,
):
    dk_acc[...] = jnp.zeros_like(dk_acc)
    dv_acc[...] = jnp.zeros_like(dv_acc)
    query_sum = jnp.zeros((1, PAIR), f32)
    for block in range(SEQ // MOST_LEN):
        rows = slice(block * MOST_LEN, (block + 1) * MOST_LEN)
        keys = slice(*key_window(block))
        grad_query = jnp.zeros((MOST_LEN, PAIR), f32)
        for head in (0, 1):
            own = own_lanes(head)
            scaled = q_ref[rows, :] * bf16(score_scale)
            query = jnp.where(own, scaled, fq_ref[rows, :])
            key = jnp.where(own, k_ref[keys, :], fk_ref[keys, :])
            scores = dot_rows(query, key)
            lane = head * HEAD_DIM
            weights = jnp.exp(scores - total_ref[rows, lane : lane + 1])
            zero = jnp.zeros((), bf16)
            grad = jnp.where(own, grad_ref[rows, :], zero)
            product = weights * dot_rows(grad, v_ref[keys, :])
            inner = jnp.sum(product, axis=-1, keepdims=True)
            grad_scores = (product - weights * inner).astype(bf16)
            grad_query += jnp.dot(
                grad_scores, jnp.where(own, k_ref[keys, :], zero), preferred_element_type=f32
            )
            dk_acc[keys, :] += dot_tokens(grad_scores, jnp.where(own, scaled, zero))
            dv_acc[keys, :] += dot_tokens(weights.astype(bf16), grad)
        grad_query *= score_scale
        query_sum += jnp.sum(grad_query, axis=0, keepdims=True)
        dq_ref[rows, :] = grad_query.astype(bf16)
    dk_ref[...] = dk_acc[...].astype(bf16)
    dv_ref[...] = dv_acc[...].astype(bf16)
    value_sum = jnp.sum(dv_acc[...], axis=0, keepdims=True)
    row = lax.broadcasted_iota(jnp.int32, (8, PAIR), 0)
    sums_ref[0, :, :] = jnp.where(row == 0, query_sum, value_sum)


def attention_specs(pairs):
    def part(index):
        return pl.BlockSpec((SEQ, PAIR), lambda r, p: (r, index * pairs + p))

    feature = pl.BlockSpec((SEQ, PAIR), lambda r, p: (r, 0))
    own = pl.BlockSpec((SEQ, PAIR), lambda r, p: (r, p))
    return [part(0), part(1), part(2), feature, feature], own


def attention_forward(project, feature_q, feature_k):
    tokens, width = project.shape[0], project.shape[1] // 3
    pairs = width // PAIR
    ins, own = attention_specs(pairs)
    return pl.pallas_call(
        attention_forward_kernel,
        grid=(tokens // SEQ, pairs),
        in_specs=ins,
        out_specs=[own, own],
        out_shape=[
            jax.ShapeDtypeStruct((tokens, width), bf16),
            jax.ShapeDtypeStruct((tokens, width), f32),
        ],
        cost_estimate=pl.CostEstimate(
            flops=4 * tokens * 3 * MOST_LEN * 2 * width,
            bytes_accessed=tokens * width * 12,
            transcendentals=tokens * 3 * MOST_LEN * width // HEAD_DIM,
        ),
        compiler_params=pltpu.CompilerParams(vmem_limit_bytes=48 << 20),
        name="attend",
    )(project, project, project, feature_q, feature_k)


def attention_backward(project, feature_q, feature_k, grad_mixed, totals):
    tokens, width = grad_mixed.shape
    pairs = width // PAIR
    ins, own = attention_specs(pairs)
    low = jax.ShapeDtypeStruct((tokens, width), bf16)
    return pl.pallas_call(
        attention_backward_kernel,
        grid=(tokens // SEQ, pairs),
        in_specs=ins + [own, own],
        out_specs=[own, own, own, pl.BlockSpec((1, 8, PAIR), lambda r, p: (r, 0, p))],
        out_shape=[low, low, low, jax.ShapeDtypeStruct((tokens // SEQ, 8, width), f32)],
        scratch_shapes=[pltpu.VMEM((SEQ, PAIR), f32), pltpu.VMEM((SEQ, PAIR), f32)],
        cost_estimate=pl.CostEstimate(
            flops=10 * tokens * 3 * MOST_LEN * 2 * width,
            bytes_accessed=tokens * width * 18,
            transcendentals=tokens * 3 * MOST_LEN * width // HEAD_DIM,
        ),
        compiler_params=pltpu.CompilerParams(vmem_limit_bytes=48 << 20),
        name="attend_back",
    )(project, project, project, feature_q, feature_k, grad_mixed, totals)


def wide_kernel(norm_ref, up_ref, branch_ref, active_ref, *rest):
    out_ref, turned, result = rest[-3:]
    piece = out_ref.shape[3]
    step = pl.program_id(0)
    for position, (left_ref, right_ref) in enumerate(
        ((norm_ref, up_ref), (branch_ref, active_ref))
    ):

        @pl.when(step == position)
        def _():
            @pl.when(pl.program_id(1) == 0)
            def _():
                turned[...] = left_ref[...].T

            result[...] = jnp.dot(turned[...], right_ref[...], preferred_element_type=f32)

    for block in range(out_ref.shape[0]):
        out_ref[block, 0, 0] = result[block * piece : (block + 1) * piece, :].astype(bf16)


def narrow_kernel(norm_ref, dq_ref, dk_ref, dv_ref, branch_ref, mixed_ref, *rest):
    out_ref, turned, result = rest[-3:]
    blocks, shards, _, piece, columns = out_ref.shape
    columns //= 4
    for position, right_ref in enumerate((dq_ref, dk_ref, dv_ref, mixed_ref)):
        if position == 0:
            turned[...] = norm_ref[...].T
        if position == 3:
            turned[...] = branch_ref[...].T
        result[...] = jnp.dot(turned[...], right_ref[...], preferred_element_type=f32)
        for block in range(blocks):
            for shard in range(shards):
                out_ref[block, shard, 0, :, position * columns : (position + 1) * columns] = (
                    result[
                        block * piece : (block + 1) * piece,
                        shard * columns : (shard + 1) * columns,
                    ].astype(bf16)
                )


def blocked_gradients(kernel, ins, in_specs, grid, out_spec, shape, store, depth, products, name):
    tokens, width = depth, shape[-1]
    alias = {}
    if store is not None:
        alias = {len(ins): 0}
        ins = ins + [store]
        in_specs = in_specs + [pl.BlockSpec(memory_space=pl.ANY)]
    return pl.pallas_call(
        kernel,
        grid=grid,
        in_specs=in_specs,
        out_specs=out_spec,
        out_shape=jax.ShapeDtypeStruct(shape, bf16),
        scratch_shapes=[pltpu.VMEM((width, tokens), bf16), pltpu.VMEM((width, width), f32)],
        input_output_aliases=alias,
        cost_estimate=pl.CostEstimate(
            flops=2 * products * tokens * width * width,
            bytes_accessed=products * 2 * (tokens * width + width * width),
            transcendentals=0,
        ),
        compiler_params=pltpu.CompilerParams(vmem_limit_bytes=56 << 20),
        name=name,
    )(*ins)


def wide_gradients(normed, grad_up, branch, active, shape, store, slot):
    tokens, width = normed.shape
    n_dp, n_tensor, _, piece, _ = shape
    whole = pl.BlockSpec((tokens, width), lambda s, t: (0, 0))
    last = n_tensor - 1
    return blocked_gradients(
        wide_kernel,
        [normed, grad_up, branch, active],
        [
            whole,
            pl.BlockSpec((tokens, width), lambda s, t: (0, jnp.where(s == 0, t, last))),
            whole,
            pl.BlockSpec((tokens, width), lambda s, t: (0, jnp.where(s == 1, t, 0))),
        ],
        (2, n_tensor),
        pl.BlockSpec((n_dp, 1, 1, piece, width), lambda s, t: (0, t, slot + s, 0, 0)),
        shape,
        store,
        tokens,
        2 * n_tensor,
        "wide_grads",
    )


def narrow_gradients(normed, grads, branch, mixed, shape, store, slot):
    tokens, width = normed.shape
    n_dp, n_tensor, _, piece, _ = shape
    whole = pl.BlockSpec((tokens, width), lambda s: (0, 0))
    return blocked_gradients(
        narrow_kernel,
        [normed, *grads, branch, mixed],
        [whole] * 6,
        (1,),
        pl.BlockSpec((n_dp, n_tensor, 1, piece, width), lambda s: (0, 0, slot, 0, 0)),
        shape,
        store,
        tokens,
        4,
        "narrow_grads",
    )


def per_device(
    tokens,
    cotangent,
    lengths,
    drop_mask,
    ln1_gain,
    ln1_bias,
    w_qkv,
    b_qv,
    w_out,
    b_out,
    ln2_gain,
    ln2_bias,
    w_up,
    b_up,
    w_down,
    b_down,
):
    layer_count = w_qkv.shape[0]
    local_rows, width = tokens.shape
    segment_count = lengths.shape[1]
    tensor_index = lax.axis_index("tensor")
    dp_index = lax.axis_index("dp")
    n_dp = lax.axis_size("dp")
    n_tensor = lax.axis_size("tensor")
    own_rows = local_rows // SEQ
    head_cols = w_qkv.shape[3]
    hidden_cols = w_up.shape[2]
    piece = width // n_dp
    out_piece = head_cols // n_dp
    hidden_piece = hidden_cols // n_dp

    own_lengths = lax.dynamic_slice_in_dim(lengths, tensor_index * own_rows, own_rows, 0)
    own_mask = lax.dynamic_slice_in_dim(drop_mask, tensor_index * own_rows, own_rows, 2)
    segment_ends = jnp.cumsum(own_lengths, axis=-1)
    positions = jnp.arange(SEQ, dtype=jnp.int32)
    segments = jnp.sum(
        (positions[None, :, None] >= segment_ends[:, None, :]).astype(jnp.int32), axis=-1
    )
    onehot = (
        segments[:, :, None] == jnp.arange(segment_count, dtype=jnp.int32)[None, None, :]
    ).astype(f32)
    keep = (
        jnp.sum(onehot[None, None] * own_mask.astype(f32)[:, :, :, None, :], axis=-1) / survival
    ).reshape(layer_count, 2, local_rows)
    lane = jnp.arange(PAIR, dtype=jnp.int32)[None, :] % HEAD_DIM
    same = segments.reshape(local_rows, 1) == lane
    feature_q = same.astype(bf16)
    feature_k = jnp.where(same | (lane >= segment_count), 0.0, masked_score).astype(bf16)

    def gather(pieces):
        rows = jnp.concatenate(pieces, axis=0)
        gathered = lax.all_gather(rows, groups, axis=0, tiled=False)
        return gathered.reshape((n_dp, n_tensor) + rows.shape)

    def part_of(array, size, axis):
        return lax.dynamic_slice_in_dim(array, dp_index * size, size, axis)

    def qkv_piece(layer):
        turned = w_qkv[layer].transpose(1, 2, 0)
        return part_of(turned, out_piece, 1).reshape(3 * out_piece, width)

    def pieces_of(layer):
        return [
            part_of(w_up[layer], hidden_piece, 1).T,
            part_of(w_down[layer], hidden_piece, 0),
            part_of(w_out[layer], out_piece, 0),
            qkv_piece(layer),
        ]

    def rows_of(got, first, count, parts=1):
        rows = got[:, :, first : first + parts * count]
        rows = rows.reshape(n_dp, n_tensor, parts, count, width).transpose(2, 1, 0, 3, 4)
        return lax.optimization_barrier(rows.reshape(parts * n_dp * n_tensor * count, width))

    def weights_of(got):
        up = rows_of(got, 0, hidden_piece)
        down = rows_of(got, hidden_piece, hidden_piece)
        out = rows_of(got, 2 * hidden_piece, out_piece)
        return rows_of(got, 2 * hidden_piece + out_piece, out_piece, 3), up, down, out

    weight_rows = 2 * hidden_piece + 4 * out_piece
    bias_rows = jnp.concatenate([b_qv.reshape(-1), b_up.reshape(-1)])
    bias_rows = jnp.pad(bias_rows, (0, 8 * width - bias_rows.shape[0])).reshape(8, width)
    full = []
    for layer in range(layer_count):
        pieces = pieces_of(layer)
        if layer == 0:
            got = gather(pieces + [bias_rows])
            all_bias = got[0, :, weight_rows:].reshape(n_tensor, 8 * width).astype(f32)
        else:
            pieces, got = lax.optimization_barrier((pieces, got))
            full.append(weights_of(got))
            got = gather(pieces)
    full.append(weights_of(got))

    qv_count = layer_count * 2 * head_cols
    bias_qv = (
        all_bias[:, :qv_count]
        .reshape(n_tensor, layer_count, 2, head_cols)
        .transpose(1, 2, 0, 3)
        .reshape(layer_count, 2, width)
    )
    bias_up = (
        all_bias[:, qv_count : qv_count + layer_count * hidden_cols]
        .reshape(n_tensor, layer_count, hidden_cols)
        .transpose(1, 0, 2)
        .reshape(layer_count, n_tensor * hidden_cols)
    )

    hidden = tokens.astype(f32)
    produced = []
    kept = []
    for layer in range(layer_count):
        normed_one, unit_one, scaled_one = norm_forward(hidden, ln1_gain[layer], ln1_bias[layer])
        normed_one = normed_one.astype(bf16)
        bias = jnp.concatenate([bias_qv[layer, 0], jnp.zeros((width,), f32), bias_qv[layer, 1]])
        full_qkv, full_up, full_down, full_out = full[layer]
        project = (dot_rows(normed_one, full_qkv) + bias).astype(bf16)
        mixed, totals = attention_forward(project, feature_q, feature_k)
        attn = jnp.dot(mixed, full_out, preferred_element_type=f32)
        middle = hidden + keep[layer, 0][:, None] * (attn + b_out[layer].astype(f32))
        normed_two, unit_two, scaled_two = norm_forward(middle, ln2_gain[layer], ln2_bias[layer])
        normed_two = normed_two.astype(bf16)
        upward = dot_rows(normed_two, full_up) + bias_up[layer]
        phi = 0.5 * (1.0 + lax.erf(upward * math.sqrt(0.5)))
        active = (upward * phi).astype(bf16)
        slope = phi + upward * (jnp.exp(-0.5 * upward * upward) * (1.0 / math.sqrt(2 * math.pi)))
        down = jnp.dot(active, full_down, preferred_element_type=f32)
        hidden = middle + keep[layer, 1][:, None] * (down + b_down[layer].astype(f32))
        produced.append(hidden.astype(bf16))
        kept.append(
            (unit_one, scaled_one, normed_one, project, totals, mixed,
             unit_two, scaled_two, normed_two, active, slope)
        )
    blocks_out = jnp.stack(produced)

    def scatter(blocks):
        flat = blocks.reshape((-1,) + blocks.shape[3:])
        flat = flat.reshape(-1, width)
        summed = lax.psum_scatter(flat, groups, scatter_dimension=0, tiled=True)
        return summed.reshape(blocks.shape[2:]).astype(f32)

    grad_flow = cotangent.astype(f32)
    collected = [None] * layer_count
    wide_slot = [None] * layer_count
    narrow_slot = [None] * layer_count
    slots = 3 * layer_count - 2
    store, taken = None, 0
    for layer in reversed(range(layer_count)):
        (unit_one, scaled_one, normed_one, project, totals, mixed,
         unit_two, scaled_two, normed_two, active, slope) = kept[layer]
        full_qkv, full_up, full_down, full_out = full[layer]
        branch_two = keep[layer, 1][:, None] * grad_flow
        grad_bias_down = jnp.sum(branch_two, axis=0)
        branch_two = branch_two.astype(bf16)
        grad_up = dot_rows(branch_two, full_down) * slope
        grad_bias_up = jnp.sum(grad_up, axis=0)
        grad_up = grad_up.astype(bf16)
        wide = (normed_two, grad_up, branch_two, active)
        if layer == layer_count - 1:
            first = wide_gradients(*wide, (n_dp, n_tensor, 2, piece, width), None, 0)
            grad_up, first = lax.optimization_barrier((grad_up, first))
            first = scatter(first)
        else:
            wide_slot[layer] = taken
            store = wide_gradients(*wide, (n_dp, n_tensor, slots, piece, width), store, taken)
            taken += 2
            grad_up, store = lax.optimization_barrier((grad_up, store))
        grad_part, grad_gain_two, grad_shift_two = norm_backward(
            jnp.dot(grad_up, full_up, preferred_element_type=f32),
            unit_two, scaled_two, ln2_gain[layer],
        )
        grad_middle = grad_flow + grad_part
        branch_one = keep[layer, 0][:, None] * grad_middle
        grad_bias_out = jnp.sum(branch_one, axis=0)
        branch_one = branch_one.astype(bf16)
        grad_mixed = dot_rows(branch_one, full_out).astype(bf16)
        *grads, sums = attention_backward(project, feature_q, feature_k, grad_mixed, totals)
        grad_bias_qv = jnp.sum(sums, axis=0)[:2]
        if layer == 0:
            first, *grads = lax.optimization_barrier((first, *grads))
        narrow_slot[layer] = taken
        store = narrow_gradients(
            normed_one, grads, branch_one, mixed,
            (n_dp, n_tensor, slots, piece, width), store, taken,
        )
        taken += 1
        grads, store = lax.optimization_barrier((grads, store))
        grad_one = sum(
            jnp.dot(
                grads[part],
                full_qkv[part * width : (part + 1) * width],
                preferred_element_type=f32,
            )
            for part in range(3)
        )
        grad_part, grad_gain_one, grad_shift_one = norm_backward(
            grad_one, unit_one, scaled_one, ln1_gain[layer]
        )
        grad_flow = grad_middle + grad_part
        collected[layer] = jnp.concatenate(
            [grad_gain_one, grad_shift_one, grad_bias_qv.reshape(-1), grad_bias_out,
             grad_gain_two, grad_shift_two, grad_bias_down, grad_bias_up]
        )
    small, later = lax.optimization_barrier((jnp.stack(collected), scatter(store)))
    small = lax.psum(small, groups)
    grad_qkv, grad_out, grad_up, grad_down = [], [], [], []
    for layer in range(layer_count):
        narrow = later[narrow_slot[layer]]
        grad_qkv.append(narrow[:, : 3 * head_cols].reshape(piece, 3, head_cols))
        grad_out.append(narrow[:, 3 * head_cols :].T)
        wide = first if layer == layer_count - 1 else later[wide_slot[layer] :]
        grad_up.append(wide[0])
        grad_down.append(wide[1].T)
    grad_qkv, grad_out, grad_up, grad_down = [
        jnp.stack(parts) for parts in (grad_qkv, grad_out, grad_up, grad_down)
    ]
    gain_one, shift_one, query_bias, value_bias, bias_out, gain_two, shift_two, bias_down = [
        small[:, position * width : (position + 1) * width] for position in range(8)
    ]
    return (
        blocks_out,
        grad_flow,
        gain_one,
        shift_one,
        grad_qkv,
        jnp.stack([query_bias, value_bias], axis=1),
        grad_out,
        bias_out,
        gain_two,
        shift_two,
        grad_up,
        small[:, 8 * width :],
        grad_down,
        bias_down,
    )


def solution(mesh):
    in_specs = (
        P(("dp", "tensor"), None),
        P(("dp", "tensor"), None),
        P("dp", None),
        P(None, None, "dp", None),
        P(),
        P(),
        P(None, None, None, "tensor"),
        P(None, None, "tensor"),
        P(None, "tensor", None),
        P(),
        P(),
        P(),
        P(None, None, "tensor"),
        P(None, "tensor"),
        P(None, "tensor", None),
        P(),
    )
    out_specs = (
        P(None, ("dp", "tensor"), None),
        P(("dp", "tensor"), None),
        P(),
        P(),
        P(None, "dp", None, "tensor"),
        P(),
        P(None, "tensor", "dp"),
        P(),
        P(),
        P(),
        P(None, "dp", "tensor"),
        P(),
        P(None, "tensor", "dp"),
        P(),
    )
    return jax.shard_map(
        per_device, mesh=mesh, in_specs=in_specs, out_specs=out_specs, check_vma=False
    )
```

```python
import math

import jax
import jax.numpy as jnp
from jax import lax
from jax.experimental import pallas as pl
from jax.experimental.pallas import tpu as pltpu
from jax.sharding import PartitionSpec as P

HEAD_DIM = 64
SEQ = 1024
MOST_LEN = 256
PAIR = 2 * HEAD_DIM

eps_norm = 1e-06
survival = 0.9
masked_score = -1e30
score_scale = 1.0 / math.sqrt(HEAD_DIM)
groups = ("dp", "tensor")
bf16 = jnp.bfloat16
f32 = jnp.float32


def norm_forward(values, norm_gain, norm_shift):
    centre = values - jnp.mean(values, axis=-1, keepdims=True)
    spread = jnp.mean(centre * centre, axis=-1, keepdims=True)
    scaled = lax.rsqrt(spread + eps_norm)
    normalized = centre * scaled
    return (normalized * norm_gain + norm_shift, normalized, scaled)


def norm_backward(grad_out, normalized, scaled, norm_gain):
    grad_unit = grad_out * norm_gain
    inner = (
        grad_unit
        - jnp.mean(grad_unit, axis=-1, keepdims=True)
        - normalized * jnp.mean(grad_unit * normalized, axis=-1, keepdims=True)
    )
    return (inner * scaled, jnp.sum(grad_out * normalized, axis=0), jnp.sum(grad_out, axis=0))


def key_window(block):
    return max(0, (block - 1) * MOST_LEN), min(SEQ, (block + 2) * MOST_LEN)


def own_lanes(head):
    lane = lax.broadcasted_iota(jnp.int32, (1, PAIR), 1)
    return lane < HEAD_DIM if head == 0 else lane >= HEAD_DIM


def dot_rows(left, right):
    return lax.dot_general(left, right, (((1,), (1,)), ((), ())), preferred_element_type=f32)


def dot_tokens(left, right):
    return lax.dot_general(left, right, (((0,), (0,)), ((), ())), preferred_element_type=f32)


def attention_forward_kernel(q_ref, k_ref, v_ref, fq_ref, fk_ref, mixed_ref, total_ref):
    for block in range(SEQ // MOST_LEN):
        rows = slice(block * MOST_LEN, (block + 1) * MOST_LEN)
        keys = slice(*key_window(block))
        mixed = []
        totals = []
        for head in (0, 1):
            own = own_lanes(head)
            query = jnp.where(own, q_ref[rows, :] * bf16(score_scale), fq_ref[rows, :])
            key = jnp.where(own, k_ref[keys, :], fk_ref[keys, :])
            scores = dot_rows(query, key)
            top = jnp.max(scores, axis=-1, keepdims=True)
            exponent = jnp.exp(scores - top)
            total = jnp.sum(exponent, axis=-1, keepdims=True)
            part = jnp.dot(exponent.astype(bf16), v_ref[keys, :], preferred_element_type=f32)
            mixed.append(part / total)
            totals.append(top + jnp.log(total))
        own = own_lanes(0)
        mixed_ref[rows, :] = jnp.where(own, mixed[0], mixed[1]).astype(bf16)
        total_ref[rows, :] = jnp.where(own, totals[0], totals[1])


def attention_backward_kernel(
    q_ref, k_ref, v_ref, fq_ref, fk_ref, grad_ref, total_ref,
    dq_ref, dk_ref, dv_ref, sums_ref, dk_acc, dv_acc,
):
    dk_acc[...] = jnp.zeros_like(dk_acc)
    dv_acc[...] = jnp.zeros_like(dv_acc)
    query_sum = jnp.zeros((1, PAIR), f32)
    for block in range(SEQ // MOST_LEN):
        rows = slice(block * MOST_LEN, (block + 1) * MOST_LEN)
        keys = slice(*key_window(block))
        grad_query = jnp.zeros((MOST_LEN, PAIR), f32)
        for head in (0, 1):
            own = own_lanes(head)
            scaled = q_ref[rows, :] * bf16(score_scale)
            query = jnp.where(own, scaled, fq_ref[rows, :])
            key = jnp.where(own, k_ref[keys, :], fk_ref[keys, :])
            scores = dot_rows(query, key)
            lane = head * HEAD_DIM
            weights = jnp.exp(scores - total_ref[rows, lane : lane + 1])
            zero = jnp.zeros((), bf16)
            grad = jnp.where(own, grad_ref[rows, :], zero)
            product = weights * dot_rows(grad, v_ref[keys, :])
            inner = jnp.sum(product, axis=-1, keepdims=True)
            grad_scores = (product - weights * inner).astype(bf16)
            grad_query += jnp.dot(
                grad_scores, jnp.where(own, k_ref[keys, :], zero), preferred_element_type=f32
            )
            dk_acc[keys, :] += dot_tokens(grad_scores, jnp.where(own, scaled, zero))
            dv_acc[keys, :] += dot_tokens(weights.astype(bf16), grad)
        grad_query *= score_scale
        query_sum += jnp.sum(grad_query, axis=0, keepdims=True)
        dq_ref[rows, :] = grad_query.astype(bf16)
    dk_ref[...] = dk_acc[...].astype(bf16)
    dv_ref[...] = dv_acc[...].astype(bf16)
    value_sum = jnp.sum(dv_acc[...], axis=0, keepdims=True)
    row = lax.broadcasted_iota(jnp.int32, (8, PAIR), 0)
    sums_ref[0, :, :] = jnp.where(row == 0, query_sum, value_sum)


def attention_specs(pairs):
    def part(index):
        return pl.BlockSpec((SEQ, PAIR), lambda r, p: (r, index * pairs + p))

    feature = pl.BlockSpec((SEQ, PAIR), lambda r, p: (r, 0))
    own = pl.BlockSpec((SEQ, PAIR), lambda r, p: (r, p))
    return [part(0), part(1), part(2), feature, feature], own


def attention_forward(project, feature_q, feature_k):
    tokens, width = project.shape[0], project.shape[1] // 3
    pairs = width // PAIR
    ins, own = attention_specs(pairs)
    return pl.pallas_call(
        attention_forward_kernel,
        grid=(tokens // SEQ, pairs),
        in_specs=ins,
        out_specs=[own, own],
        out_shape=[
            jax.ShapeDtypeStruct((tokens, width), bf16),
            jax.ShapeDtypeStruct((tokens, width), f32),
        ],
        cost_estimate=pl.CostEstimate(
            flops=4 * tokens * 3 * MOST_LEN * 2 * width,
            bytes_accessed=tokens * width * 12,
            transcendentals=tokens * 3 * MOST_LEN * width // HEAD_DIM,
        ),
        compiler_params=pltpu.CompilerParams(vmem_limit_bytes=48 << 20),
        name="attend",
    )(project, project, project, feature_q, feature_k)


def attention_backward(project, feature_q, feature_k, grad_mixed, totals):
    tokens, width = grad_mixed.shape
    pairs = width // PAIR
    ins, own = attention_specs(pairs)
    low = jax.ShapeDtypeStruct((tokens, width), bf16)
    return pl.pallas_call(
        attention_backward_kernel,
        grid=(tokens // SEQ, pairs),
        in_specs=ins + [own, own],
        out_specs=[own, own, own, pl.BlockSpec((1, 8, PAIR), lambda r, p: (r, 0, p))],
        out_shape=[low, low, low, jax.ShapeDtypeStruct((tokens // SEQ, 8, width), f32)],
        scratch_shapes=[pltpu.VMEM((SEQ, PAIR), f32), pltpu.VMEM((SEQ, PAIR), f32)],
        cost_estimate=pl.CostEstimate(
            flops=10 * tokens * 3 * MOST_LEN * 2 * width,
            bytes_accessed=tokens * width * 18,
            transcendentals=tokens * 3 * MOST_LEN * width // HEAD_DIM,
        ),
        compiler_params=pltpu.CompilerParams(vmem_limit_bytes=48 << 20),
        name="attend_back",
    )(project, project, project, feature_q, feature_k, grad_mixed, totals)


def unpack_kernel(got_ref, qkv_ref, up_ref, down_ref, out_ref):
    blocks, hidden, few = up_ref.shape[1], up_ref.shape[2], out_ref.shape[2]
    for block in range(blocks):
        up_ref[0, block] = got_ref[block, 0, :hidden, :]
        down_ref[0, block] = got_ref[block, 0, hidden : 2 * hidden, :]
        out_ref[0, block] = got_ref[block, 0, 2 * hidden : 2 * hidden + few, :]
        for part in range(3):
            first = 2 * hidden + (1 + part) * few
            qkv_ref[part, 0, block] = got_ref[block, 0, first : first + few, :]


def unpack(got, hidden, few):
    n_dp, n_tensor, rows, width = got.shape

    def spec(count):
        return pl.BlockSpec((1, n_dp, count, width), lambda t: (t, 0, 0, 0))

    def shape(count):
        return jax.ShapeDtypeStruct((n_tensor, n_dp, count, width), bf16)

    outs = pl.pallas_call(
        unpack_kernel,
        grid=(n_tensor,),
        in_specs=[pl.BlockSpec((n_dp, 1, rows, width), lambda t: (0, t, 0, 0))],
        out_specs=[
            pl.BlockSpec((3, 1, n_dp, few, width), lambda t: (0, t, 0, 0, 0)),
            spec(hidden),
            spec(hidden),
            spec(few),
        ],
        out_shape=[
            jax.ShapeDtypeStruct((3, n_tensor, n_dp, few, width), bf16),
            shape(hidden),
            shape(hidden),
            shape(few),
        ],
        cost_estimate=pl.CostEstimate(
            flops=0, bytes_accessed=4 * n_dp * n_tensor * rows * width, transcendentals=0
        ),
        compiler_params=pltpu.CompilerParams(vmem_limit_bytes=48 << 20),
        name="unpack",
    )(got)
    return [array.reshape(-1, width) for array in outs]


def sum_over(values, axis, size):
    if size & (size - 1):
        return lax.psum(values, axis)
    reach = 1
    while reach < size:
        pairs = [(index, index ^ reach) for index in range(size)]
        values = values + lax.ppermute(values, axis, pairs)
        reach *= 2
    return values


def wide_kernel(norm_ref, up_ref, branch_ref, active_ref, *rest):
    out_ref, turned, result = rest[-3:]
    piece = out_ref.shape[3]
    step = pl.program_id(0)
    for position, (left_ref, right_ref) in enumerate(
        ((norm_ref, up_ref), (branch_ref, active_ref))
    ):

        @pl.when(step == position)
        def _():
            @pl.when(pl.program_id(1) == 0)
            def _():
                turned[...] = left_ref[...].T

            result[...] = jnp.dot(turned[...], right_ref[...], preferred_element_type=f32)

    for block in range(out_ref.shape[0]):
        out_ref[block, 0, 0] = result[block * piece : (block + 1) * piece, :].astype(bf16)


def narrow_kernel(norm_ref, dq_ref, dk_ref, dv_ref, branch_ref, mixed_ref, *rest):
    out_ref, turned, result = rest[-3:]
    blocks, shards, _, piece, columns = out_ref.shape
    columns //= 4
    for position, right_ref in enumerate((dq_ref, dk_ref, dv_ref, mixed_ref)):
        if position == 0:
            turned[...] = norm_ref[...].T
        if position == 3:
            turned[...] = branch_ref[...].T
        result[...] = jnp.dot(turned[...], right_ref[...], preferred_element_type=f32)
        for block in range(blocks):
            for shard in range(shards):
                out_ref[block, shard, 0, :, position * columns : (position + 1) * columns] = (
                    result[
                        block * piece : (block + 1) * piece,
                        shard * columns : (shard + 1) * columns,
                    ].astype(bf16)
                )


def blocked_gradients(kernel, ins, in_specs, grid, out_spec, shape, store, depth, products, name):
    tokens, width = depth, shape[-1]
    alias = {}
    if store is not None:
        alias = {len(ins): 0}
        ins = ins + [store]
        in_specs = in_specs + [pl.BlockSpec(memory_space=pl.ANY)]
    return pl.pallas_call(
        kernel,
        grid=grid,
        in_specs=in_specs,
        out_specs=out_spec,
        out_shape=jax.ShapeDtypeStruct(shape, bf16),
        scratch_shapes=[pltpu.VMEM((width, tokens), bf16), pltpu.VMEM((width, width), f32)],
        input_output_aliases=alias,
        cost_estimate=pl.CostEstimate(
            flops=2 * products * tokens * width * width,
            bytes_accessed=products * 2 * (tokens * width + width * width),
            transcendentals=0,
        ),
        compiler_params=pltpu.CompilerParams(vmem_limit_bytes=56 << 20),
        name=name,
    )(*ins)


def wide_gradients(normed, grad_up, branch, active, shape, store, slot):
    tokens, width = normed.shape
    n_dp, n_tensor, _, piece, _ = shape
    whole = pl.BlockSpec((tokens, width), lambda s, t: (0, 0))
    last = n_tensor - 1
    return blocked_gradients(
        wide_kernel,
        [normed, grad_up, branch, active],
        [
            whole,
            pl.BlockSpec((tokens, width), lambda s, t: (0, jnp.where(s == 0, t, last))),
            whole,
            pl.BlockSpec((tokens, width), lambda s, t: (0, jnp.where(s == 1, t, 0))),
        ],
        (2, n_tensor),
        pl.BlockSpec((n_dp, 1, 1, piece, width), lambda s, t: (0, t, slot + s, 0, 0)),
        shape,
        store,
        tokens,
        2 * n_tensor,
        "wide_grads",
    )


def narrow_gradients(normed, grads, branch, mixed, shape, store, slot):
    tokens, width = normed.shape
    n_dp, n_tensor, _, piece, _ = shape
    whole = pl.BlockSpec((tokens, width), lambda s: (0, 0))
    return blocked_gradients(
        narrow_kernel,
        [normed, *grads, branch, mixed],
        [whole] * 6,
        (1,),
        pl.BlockSpec((n_dp, n_tensor, 1, piece, width), lambda s: (0, 0, slot, 0, 0)),
        shape,
        store,
        tokens,
        4,
        "narrow_grads",
    )


def per_device(
    tokens,
    cotangent,
    lengths,
    drop_mask,
    ln1_gain,
    ln1_bias,
    w_qkv,
    b_qv,
    w_out,
    b_out,
    ln2_gain,
    ln2_bias,
    w_up,
    b_up,
    w_down,
    b_down,
):
    layer_count = w_qkv.shape[0]
    local_rows, width = tokens.shape
    segment_count = lengths.shape[1]
    tensor_index = lax.axis_index("tensor")
    dp_index = lax.axis_index("dp")
    n_dp = lax.axis_size("dp")
    n_tensor = lax.axis_size("tensor")
    own_rows = local_rows // SEQ
    head_cols = w_qkv.shape[3]
    hidden_cols = w_up.shape[2]
    piece = width // n_dp
    out_piece = head_cols // n_dp
    hidden_piece = hidden_cols // n_dp

    own_lengths = lax.dynamic_slice_in_dim(lengths, tensor_index * own_rows, own_rows, 0)
    own_mask = lax.dynamic_slice_in_dim(drop_mask, tensor_index * own_rows, own_rows, 2)
    segment_ends = jnp.cumsum(own_lengths, axis=-1)
    positions = jnp.arange(SEQ, dtype=jnp.int32)
    segments = jnp.sum(
        (positions[None, :, None] >= segment_ends[:, None, :]).astype(jnp.int32), axis=-1
    )
    onehot = (
        segments[:, :, None] == jnp.arange(segment_count, dtype=jnp.int32)[None, None, :]
    ).astype(f32)
    keep = (
        jnp.sum(onehot[None, None] * own_mask.astype(f32)[:, :, :, None, :], axis=-1) / survival
    ).reshape(layer_count, 2, local_rows)
    lane = jnp.arange(PAIR, dtype=jnp.int32)[None, :] % HEAD_DIM
    same = segments.reshape(local_rows, 1) == lane
    feature_q = same.astype(bf16)
    feature_k = jnp.where(same | (lane >= segment_count), 0.0, masked_score).astype(bf16)

    def gather(pieces):
        rows = jnp.concatenate(pieces, axis=0)
        gathered = lax.all_gather(rows, groups, axis=0, tiled=False)
        return gathered.reshape((n_dp, n_tensor) + rows.shape)

    def part_of(array, size, axis):
        return lax.dynamic_slice_in_dim(array, dp_index * size, size, axis)

    def qkv_piece(layer):
        turned = w_qkv[layer].transpose(1, 2, 0)
        return part_of(turned, out_piece, 1).reshape(3 * out_piece, width)

    def pieces_of(layer):
        return [
            part_of(w_up[layer], hidden_piece, 1).T,
            part_of(w_down[layer], hidden_piece, 0),
            part_of(w_out[layer], out_piece, 0),
            qkv_piece(layer),
        ]

    def rows_of(got, first, count, parts=1):
        rows = got[:, :, first : first + parts * count]
        rows = rows.reshape(n_dp, n_tensor, parts, count, width).transpose(2, 1, 0, 3, 4)
        return lax.optimization_barrier(rows.reshape(parts * n_dp * n_tensor * count, width))

    def weights_of(got):
        if piece % 16 == 0 and hidden_piece == piece and out_piece % 8 == 0:
            return unpack(got, hidden_piece, out_piece)
        up = rows_of(got, 0, hidden_piece)
        down = rows_of(got, hidden_piece, hidden_piece)
        out = rows_of(got, 2 * hidden_piece, out_piece)
        return rows_of(got, 2 * hidden_piece + out_piece, out_piece, 3), up, down, out

    weight_rows = 2 * hidden_piece + 4 * out_piece
    bias_rows = jnp.concatenate([b_qv.reshape(-1), b_up.reshape(-1)])
    bias_rows = jnp.pad(bias_rows, (0, 8 * width - bias_rows.shape[0])).reshape(8, width)
    full = []
    for layer in range(layer_count):
        pieces = pieces_of(layer)
        if layer == 0:
            got = gather(pieces + [bias_rows])
            all_bias = got[0, :, weight_rows:].reshape(n_tensor, 8 * width).astype(f32)
        else:
            pieces, got = lax.optimization_barrier((pieces, got))
            full.append(weights_of(got))
            got = gather(pieces)
    full.append(weights_of(got))

    qv_count = layer_count * 2 * head_cols
    bias_qv = (
        all_bias[:, :qv_count]
        .reshape(n_tensor, layer_count, 2, head_cols)
        .transpose(1, 2, 0, 3)
        .reshape(layer_count, 2, width)
    )
    bias_up = (
        all_bias[:, qv_count : qv_count + layer_count * hidden_cols]
        .reshape(n_tensor, layer_count, hidden_cols)
        .transpose(1, 0, 2)
        .reshape(layer_count, n_tensor * hidden_cols)
    )

    hidden = tokens.astype(f32)
    produced = []
    kept = []
    for layer in range(layer_count):
        normed_one, unit_one, scaled_one = norm_forward(hidden, ln1_gain[layer], ln1_bias[layer])
        normed_one = normed_one.astype(bf16)
        bias = jnp.concatenate([bias_qv[layer, 0], jnp.zeros((width,), f32), bias_qv[layer, 1]])
        full_qkv, full_up, full_down, full_out = full[layer]
        project = (dot_rows(normed_one, full_qkv) + bias).astype(bf16)
        mixed, totals = attention_forward(project, feature_q, feature_k)
        attn = jnp.dot(mixed, full_out, preferred_element_type=f32)
        middle = hidden + keep[layer, 0][:, None] * (attn + b_out[layer].astype(f32))
        normed_two, unit_two, scaled_two = norm_forward(middle, ln2_gain[layer], ln2_bias[layer])
        normed_two = normed_two.astype(bf16)
        upward = dot_rows(normed_two, full_up) + bias_up[layer]
        phi = 0.5 * (1.0 + lax.erf(upward * math.sqrt(0.5)))
        active = (upward * phi).astype(bf16)
        slope = phi + upward * (jnp.exp(-0.5 * upward * upward) * (1.0 / math.sqrt(2 * math.pi)))
        down = jnp.dot(active, full_down, preferred_element_type=f32)
        hidden = middle + keep[layer, 1][:, None] * (down + b_down[layer].astype(f32))
        produced.append(hidden.astype(bf16))
        kept.append(
            (unit_one, scaled_one, normed_one, project, totals, mixed,
             unit_two, scaled_two, normed_two, active, slope)
        )
    blocks_out = jnp.stack(produced)

    def scatter(blocks):
        flat = blocks.reshape((-1,) + blocks.shape[3:])
        flat = flat.reshape(-1, width)
        summed = lax.psum_scatter(flat, groups, scatter_dimension=0, tiled=True)
        return summed.reshape(blocks.shape[2:]).astype(f32)

    grad_flow = cotangent.astype(f32)
    collected = [None] * layer_count
    wide_slot = [None] * layer_count
    narrow_slot = [None] * layer_count
    slots = 3 * layer_count - 2
    store, taken = None, 0
    for layer in reversed(range(layer_count)):
        (unit_one, scaled_one, normed_one, project, totals, mixed,
         unit_two, scaled_two, normed_two, active, slope) = kept[layer]
        full_qkv, full_up, full_down, full_out = full[layer]
        branch_two = keep[layer, 1][:, None] * grad_flow
        grad_bias_down = jnp.sum(branch_two, axis=0)
        branch_two = branch_two.astype(bf16)
        grad_up = dot_rows(branch_two, full_down) * slope
        grad_bias_up = jnp.sum(grad_up, axis=0)
        grad_up = grad_up.astype(bf16)
        wide = (normed_two, grad_up, branch_two, active)
        if layer == layer_count - 1:
            first = wide_gradients(*wide, (n_dp, n_tensor, 2, piece, width), None, 0)
            grad_up, first = lax.optimization_barrier((grad_up, first))
            first = scatter(first)
        else:
            wide_slot[layer] = taken
            store = wide_gradients(*wide, (n_dp, n_tensor, slots, piece, width), store, taken)
            taken += 2
            grad_up, store = lax.optimization_barrier((grad_up, store))
        grad_part, grad_gain_two, grad_shift_two = norm_backward(
            jnp.dot(grad_up, full_up, preferred_element_type=f32),
            unit_two, scaled_two, ln2_gain[layer],
        )
        grad_middle = grad_flow + grad_part
        branch_one = keep[layer, 0][:, None] * grad_middle
        grad_bias_out = jnp.sum(branch_one, axis=0)
        branch_one = branch_one.astype(bf16)
        grad_mixed = dot_rows(branch_one, full_out).astype(bf16)
        *grads, sums = attention_backward(project, feature_q, feature_k, grad_mixed, totals)
        grad_bias_qv = jnp.sum(sums, axis=0)[:2]
        if layer == 0:
            first, *grads = lax.optimization_barrier((first, *grads))
        narrow_slot[layer] = taken
        store = narrow_gradients(
            normed_one, grads, branch_one, mixed,
            (n_dp, n_tensor, slots, piece, width), store, taken,
        )
        taken += 1
        grads, store = lax.optimization_barrier((grads, store))
        grad_one = sum(
            jnp.dot(
                grads[part],
                full_qkv[part * width : (part + 1) * width],
                preferred_element_type=f32,
            )
            for part in range(3)
        )
        grad_part, grad_gain_one, grad_shift_one = norm_backward(
            grad_one, unit_one, scaled_one, ln1_gain[layer]
        )
        grad_flow = grad_middle + grad_part
        collected[layer] = jnp.concatenate(
            [grad_gain_one, grad_shift_one, grad_bias_qv.reshape(-1), grad_bias_out,
             grad_gain_two, grad_shift_two, grad_bias_down, grad_bias_up]
        )
    later = scatter(store)
    small = jnp.stack(collected)
    for axis in groups:
        small = sum_over(small, axis, lax.axis_size(axis))
    grad_qkv, grad_out, grad_up, grad_down = [], [], [], []
    for layer in range(layer_count):
        narrow = later[narrow_slot[layer]]
        grad_qkv.append(narrow[:, : 3 * head_cols].reshape(piece, 3, head_cols))
        grad_out.append(narrow[:, 3 * head_cols :].T)
        wide = first if layer == layer_count - 1 else later[wide_slot[layer] :]
        grad_up.append(wide[0])
        grad_down.append(wide[1].T)
    grad_qkv, grad_out, grad_up, grad_down = [
        jnp.stack(parts) for parts in (grad_qkv, grad_out, grad_up, grad_down)
    ]
    gain_one, shift_one, query_bias, value_bias, bias_out, gain_two, shift_two, bias_down = [
        small[:, position * width : (position + 1) * width] for position in range(8)
    ]
    return (
        blocks_out,
        grad_flow,
        gain_one,
        shift_one,
        grad_qkv,
        jnp.stack([query_bias, value_bias], axis=1),
        grad_out,
        bias_out,
        gain_two,
        shift_two,
        grad_up,
        small[:, 8 * width :],
        grad_down,
        bias_down,
    )


def solution(mesh):
    in_specs = (
        P(("dp", "tensor"), None),
        P(("dp", "tensor"), None),
        P("dp", None),
        P(None, None, "dp", None),
        P(),
        P(),
        P(None, None, None, "tensor"),
        P(None, None, "tensor"),
        P(None, "tensor", None),
        P(),
        P(),
        P(),
        P(None, None, "tensor"),
        P(None, "tensor"),
        P(None, "tensor", None),
        P(),
    )
    out_specs = (
        P(None, ("dp", "tensor"), None),
        P(("dp", "tensor"), None),
        P(),
        P(),
        P(None, "dp", None, "tensor"),
        P(),
        P(None, "tensor", "dp"),
        P(),
        P(),
        P(),
        P(None, "dp", "tensor"),
        P(),
        P(None, "tensor", "dp"),
        P(),
    )
    return jax.shard_map(
        per_device, mesh=mesh, in_specs=in_specs, out_specs=out_specs, check_vma=False
    )
```

```python
import math

import jax
import jax.numpy as jnp
from jax import lax
from jax.experimental import pallas as pl
from jax.experimental.pallas import tpu as pltpu
from jax.sharding import PartitionSpec as P

HEAD_DIM = 64
SEQ = 1024
MOST_LEN = 256
PAIR = 2 * HEAD_DIM

eps_norm = 1e-06
survival = 0.9
masked_score = -1e30
score_scale = 1.0 / math.sqrt(HEAD_DIM)
groups = ("dp", "tensor")
bf16 = jnp.bfloat16
f32 = jnp.float32


def norm_forward(values, norm_gain, norm_shift):
    centre = values - jnp.mean(values, axis=-1, keepdims=True)
    spread = jnp.mean(centre * centre, axis=-1, keepdims=True)
    scaled = lax.rsqrt(spread + eps_norm)
    normalized = centre * scaled
    return (normalized * norm_gain + norm_shift, normalized, scaled)


def norm_backward(grad_out, normalized, scaled, norm_gain):
    grad_unit = grad_out * norm_gain
    inner = (
        grad_unit
        - jnp.mean(grad_unit, axis=-1, keepdims=True)
        - normalized * jnp.mean(grad_unit * normalized, axis=-1, keepdims=True)
    )
    return (inner * scaled, jnp.sum(grad_out * normalized, axis=0), jnp.sum(grad_out, axis=0))


def key_window(block):
    return max(0, (block - 1) * MOST_LEN), min(SEQ, (block + 2) * MOST_LEN)


def own_lanes(head):
    lane = lax.broadcasted_iota(jnp.int32, (1, PAIR), 1)
    return lane < HEAD_DIM if head == 0 else lane >= HEAD_DIM


def dot_rows(left, right):
    return lax.dot_general(left, right, (((1,), (1,)), ((), ())), preferred_element_type=f32)


def dot_tokens(left, right):
    return lax.dot_general(left, right, (((0,), (0,)), ((), ())), preferred_element_type=f32)


def attention_forward_kernel(q_ref, k_ref, v_ref, fq_ref, fk_ref, mixed_ref, total_ref):
    for block in range(SEQ // MOST_LEN):
        rows = slice(block * MOST_LEN, (block + 1) * MOST_LEN)
        keys = slice(*key_window(block))
        mixed = []
        totals = []
        for head in (0, 1):
            own = own_lanes(head)
            query = jnp.where(own, q_ref[rows, :] * bf16(score_scale), fq_ref[rows, :])
            key = jnp.where(own, k_ref[keys, :], fk_ref[keys, :])
            scores = dot_rows(query, key)
            top = jnp.max(scores, axis=-1, keepdims=True)
            exponent = jnp.exp(scores - top)
            total = jnp.sum(exponent, axis=-1, keepdims=True)
            part = jnp.dot(exponent.astype(bf16), v_ref[keys, :], preferred_element_type=f32)
            mixed.append(part / total)
            totals.append(top + jnp.log(total))
        own = own_lanes(0)
        mixed_ref[rows, :] = jnp.where(own, mixed[0], mixed[1]).astype(bf16)
        total_ref[rows, :] = jnp.where(own, totals[0], totals[1])


def attention_backward_kernel(
    q_ref, k_ref, v_ref, fq_ref, fk_ref, grad_ref, total_ref,
    dq_ref, dk_ref, dv_ref, sums_ref, dk_acc, dv_acc,
):
    dk_acc[...] = jnp.zeros_like(dk_acc)
    dv_acc[...] = jnp.zeros_like(dv_acc)
    query_sum = jnp.zeros((1, PAIR), f32)
    for block in range(SEQ // MOST_LEN):
        rows = slice(block * MOST_LEN, (block + 1) * MOST_LEN)
        keys = slice(*key_window(block))
        grad_query = jnp.zeros((MOST_LEN, PAIR), f32)
        for head in (0, 1):
            own = own_lanes(head)
            scaled = q_ref[rows, :] * bf16(score_scale)
            query = jnp.where(own, scaled, fq_ref[rows, :])
            key = jnp.where(own, k_ref[keys, :], fk_ref[keys, :])
            scores = dot_rows(query, key)
            lane = head * HEAD_DIM
            weights = jnp.exp(scores - total_ref[rows, lane : lane + 1])
            zero = jnp.zeros((), bf16)
            grad = jnp.where(own, grad_ref[rows, :], zero)
            product = weights * dot_rows(grad, v_ref[keys, :])
            inner = jnp.sum(product, axis=-1, keepdims=True)
            grad_scores = (product - weights * inner).astype(bf16)
            grad_query += jnp.dot(
                grad_scores, jnp.where(own, k_ref[keys, :], zero), preferred_element_type=f32
            )
            dk_acc[keys, :] += dot_tokens(grad_scores, jnp.where(own, scaled, zero))
            dv_acc[keys, :] += dot_tokens(weights.astype(bf16), grad)
        grad_query *= score_scale
        query_sum += jnp.sum(grad_query, axis=0, keepdims=True)
        dq_ref[rows, :] = grad_query.astype(bf16)
    dk_ref[...] = dk_acc[...].astype(bf16)
    dv_ref[...] = dv_acc[...].astype(bf16)
    value_sum = jnp.sum(dv_acc[...], axis=0, keepdims=True)
    row = lax.broadcasted_iota(jnp.int32, (8, PAIR), 0)
    sums_ref[0, :, :] = jnp.where(row == 0, query_sum, value_sum)


def attention_specs(pairs):
    def part(index):
        return pl.BlockSpec((SEQ, PAIR), lambda r, p: (r, index * pairs + p))

    feature = pl.BlockSpec((SEQ, PAIR), lambda r, p: (r, 0))
    own = pl.BlockSpec((SEQ, PAIR), lambda r, p: (r, p))
    return [part(0), part(1), part(2), feature, feature], own


def attention_forward(project, feature_q, feature_k):
    tokens, width = project.shape[0], project.shape[1] // 3
    pairs = width // PAIR
    ins, own = attention_specs(pairs)
    return pl.pallas_call(
        attention_forward_kernel,
        grid=(tokens // SEQ, pairs),
        in_specs=ins,
        out_specs=[own, own],
        out_shape=[
            jax.ShapeDtypeStruct((tokens, width), bf16),
            jax.ShapeDtypeStruct((tokens, width), f32),
        ],
        cost_estimate=pl.CostEstimate(
            flops=4 * tokens * 3 * MOST_LEN * 2 * width,
            bytes_accessed=tokens * width * 12,
            transcendentals=tokens * 3 * MOST_LEN * width // HEAD_DIM,
        ),
        compiler_params=pltpu.CompilerParams(vmem_limit_bytes=48 << 20),
        name="attend",
    )(project, project, project, feature_q, feature_k)


def attention_backward(project, feature_q, feature_k, grad_mixed, totals):
    tokens, width = grad_mixed.shape
    pairs = width // PAIR
    ins, own = attention_specs(pairs)
    low = jax.ShapeDtypeStruct((tokens, width), bf16)
    return pl.pallas_call(
        attention_backward_kernel,
        grid=(tokens // SEQ, pairs),
        in_specs=ins + [own, own],
        out_specs=[own, own, own, pl.BlockSpec((1, 8, PAIR), lambda r, p: (r, 0, p))],
        out_shape=[low, low, low, jax.ShapeDtypeStruct((tokens // SEQ, 8, width), f32)],
        scratch_shapes=[pltpu.VMEM((SEQ, PAIR), f32), pltpu.VMEM((SEQ, PAIR), f32)],
        cost_estimate=pl.CostEstimate(
            flops=10 * tokens * 3 * MOST_LEN * 2 * width,
            bytes_accessed=tokens * width * 18,
            transcendentals=tokens * 3 * MOST_LEN * width // HEAD_DIM,
        ),
        compiler_params=pltpu.CompilerParams(vmem_limit_bytes=48 << 20),
        name="attend_back",
    )(project, project, project, feature_q, feature_k, grad_mixed, totals)


def unpack_kernel(got_ref, qkv_ref, up_ref, down_ref, out_ref):
    blocks, hidden, few = up_ref.shape[1], up_ref.shape[2], out_ref.shape[2]
    for block in range(blocks):
        up_ref[0, block] = got_ref[block, 0, :hidden, :]
        down_ref[0, block] = got_ref[block, 0, hidden : 2 * hidden, :]
        out_ref[0, block] = got_ref[block, 0, 2 * hidden : 2 * hidden + few, :]
        for part in range(3):
            first = 2 * hidden + (1 + part) * few
            qkv_ref[part, 0, block] = got_ref[block, 0, first : first + few, :]


def unpack(got, hidden, few):
    n_dp, n_tensor, rows, width = got.shape

    def spec(count):
        return pl.BlockSpec((1, n_dp, count, width), lambda t: (t, 0, 0, 0))

    def shape(count):
        return jax.ShapeDtypeStruct((n_tensor, n_dp, count, width), bf16)

    outs = pl.pallas_call(
        unpack_kernel,
        grid=(n_tensor,),
        in_specs=[pl.BlockSpec((n_dp, 1, rows, width), lambda t: (0, t, 0, 0))],
        out_specs=[
            pl.BlockSpec((3, 1, n_dp, few, width), lambda t: (0, t, 0, 0, 0)),
            spec(hidden),
            spec(hidden),
            spec(few),
        ],
        out_shape=[
            jax.ShapeDtypeStruct((3, n_tensor, n_dp, few, width), bf16),
            shape(hidden),
            shape(hidden),
            shape(few),
        ],
        cost_estimate=pl.CostEstimate(
            flops=0, bytes_accessed=4 * n_dp * n_tensor * rows * width, transcendentals=0
        ),
        compiler_params=pltpu.CompilerParams(vmem_limit_bytes=48 << 20),
        name="unpack",
    )(got)
    return [array.reshape(-1, width) for array in outs]


def sum_over(values, axis, size):
    if size & (size - 1):
        return lax.psum(values, axis)
    reach = 1
    while reach < size:
        pairs = [(index, index ^ reach) for index in range(size)]
        values = values + lax.ppermute(values, axis, pairs)
        reach *= 2
    return values


class PermuteScatter:
    def __init__(self, blocks, order):
        self.bits = {axis: lax.axis_size(axis).bit_length() - 1 for axis in groups}
        self.left = [(axis, bit) for axis in groups for bit in reversed(range(self.bits[axis]))]
        self.blocks = blocks.reshape((2,) * len(self.left) + blocks.shape[2:])
        self.steps = order(self.bits)

    def step(self, count=1):
        for axis, bit in self.steps[:count]:
            dim = self.left.index((axis, bit))
            self.left.pop(dim)
            side = (lax.axis_index(axis) >> bit) & 1
            sent = lax.dynamic_index_in_dim(self.blocks, 1 - side, dim, keepdims=False)
            own = lax.dynamic_index_in_dim(self.blocks, side, dim, keepdims=False)
            pairs = [(index, index ^ (1 << bit)) for index in range(1 << self.bits[axis])]
            blocks = own.astype(f32) + lax.ppermute(sent, axis, pairs).astype(f32)
            self.blocks = blocks.astype(bf16) if self.left else blocks
        self.steps = self.steps[count:]

    def finish(self):
        self.step(len(self.steps))
        return self.blocks


def tie(value, chains):
    value, blocks = lax.optimization_barrier((value, [chain.blocks for chain in chains]))
    for chain, block in zip(chains, blocks):
        chain.blocks = block
    return value


def advance(value, chains):
    for chain in chains:
        chain.step()
    return tie(value, chains)


def rising(bits):
    return [(axis, bit) for axis in groups for bit in range(bits[axis])]


def turned_about(bits):
    steps = rising(bits)
    count = bits[groups[0]]
    return steps[:1] + steps[1:count][::-1] + steps[count:]


def wide_kernel(norm_ref, up_ref, branch_ref, active_ref, *rest):
    *out_refs, turned, result = rest
    piece = out_refs[0].shape[3]
    step = pl.program_id(0)
    for position, (left_ref, right_ref) in enumerate(
        ((norm_ref, up_ref), (branch_ref, active_ref))
    ):
        out_ref = out_refs[position % len(out_refs)]

        @pl.when(step == position)
        def _():
            @pl.when(pl.program_id(1) == 0)
            def _():
                turned[...] = left_ref[...].T

            result[...] = jnp.dot(turned[...], right_ref[...], preferred_element_type=f32)
            for block in range(out_ref.shape[0]):
                out_ref[block, 0, 0] = result[block * piece : (block + 1) * piece, :].astype(bf16)


def narrow_kernel(
    norm_ref, dq_ref, dk_ref, dv_ref, branch_ref, mixed_ref,
    out_ref, turned, result,
):
    blocks, shards, _, piece, columns = out_ref.shape
    columns //= 4
    for position, right_ref in enumerate((dq_ref, dk_ref, dv_ref, mixed_ref)):
        if position == 0:
            turned[...] = norm_ref[...].T
        if position == 3:
            turned[...] = branch_ref[...].T
        result[...] = jnp.dot(turned[...], right_ref[...], preferred_element_type=f32)
        for block in range(blocks):
            for shard in range(shards):
                out_ref[block, shard, 0, :, position * columns : (position + 1) * columns] = (
                    result[
                        block * piece : (block + 1) * piece,
                        shard * columns : (shard + 1) * columns,
                    ].astype(bf16)
                )


def blocked_gradients(kernel, ins, in_specs, grid, out_spec, shape, products, name):
    tokens, width = ins[0].shape
    return pl.pallas_call(
        kernel,
        grid=grid,
        in_specs=in_specs,
        out_specs=out_spec,
        out_shape=[jax.ShapeDtypeStruct(shape, bf16)] * len(out_spec),
        scratch_shapes=[pltpu.VMEM((width, tokens), bf16), pltpu.VMEM((width, width), f32)],
        cost_estimate=pl.CostEstimate(
            flops=2 * products * tokens * width * width,
            bytes_accessed=products * 2 * (tokens * width + width * width),
            transcendentals=0,
        ),
        compiler_params=pltpu.CompilerParams(vmem_limit_bytes=56 << 20),
        name=name,
    )(*ins)


def wide_gradients(normed, grad_up, branch, active, shape, split):
    tokens, width = normed.shape
    n_dp, n_tensor, _, piece, _ = shape
    whole = pl.BlockSpec((tokens, width), lambda s, t: (0, 0))
    last = n_tensor - 1
    if split:
        indices = [
            lambda s, t: (0, jnp.where(s == 0, t, last), 0, 0, 0),
            lambda s, t: (0, jnp.where(s == 1, t, 0), 0, 0, 0),
        ]
    else:
        indices = [lambda s, t: (0, t, s, 0, 0)]
    return blocked_gradients(
        wide_kernel,
        [normed, grad_up, branch, active],
        [
            whole,
            pl.BlockSpec((tokens, width), lambda s, t: (0, jnp.where(s == 0, t, last))),
            whole,
            pl.BlockSpec((tokens, width), lambda s, t: (0, jnp.where(s == 1, t, 0))),
        ],
        (2, n_tensor),
        [pl.BlockSpec((n_dp, 1, 1, piece, width), index) for index in indices],
        shape[:2] + (1 if split else 2,) + shape[3:],
        2 * n_tensor,
        "wide_grads",
    )


def narrow_gradients(normed, grads, branch, mixed, shape):
    tokens, width = normed.shape
    n_dp, n_tensor, _, piece, _ = shape
    whole = pl.BlockSpec((tokens, width), lambda s: (0, 0))
    return blocked_gradients(
        narrow_kernel,
        [normed, *grads, branch, mixed],
        [whole] * 6,
        (1,),
        [pl.BlockSpec((n_dp, n_tensor, 1, piece, width), lambda s: (0, 0, 0, 0, 0))],
        shape,
        4,
        "narrow_grads",
    )


def per_device(
    tokens,
    cotangent,
    lengths,
    drop_mask,
    ln1_gain,
    ln1_bias,
    w_qkv,
    b_qv,
    w_out,
    b_out,
    ln2_gain,
    ln2_bias,
    w_up,
    b_up,
    w_down,
    b_down,
):
    layer_count = w_qkv.shape[0]
    local_rows, width = tokens.shape
    segment_count = lengths.shape[1]
    tensor_index = lax.axis_index("tensor")
    dp_index = lax.axis_index("dp")
    n_dp = lax.axis_size("dp")
    n_tensor = lax.axis_size("tensor")
    own_rows = local_rows // SEQ
    head_cols = w_qkv.shape[3]
    hidden_cols = w_up.shape[2]
    piece = width // n_dp
    out_piece = head_cols // n_dp
    hidden_piece = hidden_cols // n_dp

    own_lengths = lax.dynamic_slice_in_dim(lengths, tensor_index * own_rows, own_rows, 0)
    own_mask = lax.dynamic_slice_in_dim(drop_mask, tensor_index * own_rows, own_rows, 2)
    segment_ends = jnp.cumsum(own_lengths, axis=-1)
    positions = jnp.arange(SEQ, dtype=jnp.int32)
    segments = jnp.sum(
        (positions[None, :, None] >= segment_ends[:, None, :]).astype(jnp.int32), axis=-1
    )
    onehot = (
        segments[:, :, None] == jnp.arange(segment_count, dtype=jnp.int32)[None, None, :]
    ).astype(f32)
    keep = (
        jnp.sum(onehot[None, None] * own_mask.astype(f32)[:, :, :, None, :], axis=-1) / survival
    ).reshape(layer_count, 2, local_rows)
    lane = jnp.arange(PAIR, dtype=jnp.int32)[None, :] % HEAD_DIM
    same = segments.reshape(local_rows, 1) == lane
    feature_q = same.astype(bf16)
    feature_k = jnp.where(same | (lane >= segment_count), 0.0, masked_score).astype(bf16)

    def gather(pieces):
        rows = jnp.concatenate(pieces, axis=0)
        gathered = lax.all_gather(rows, groups, axis=0, tiled=False)
        return gathered.reshape((n_dp, n_tensor) + rows.shape)

    def part_of(array, size, axis):
        return lax.dynamic_slice_in_dim(array, dp_index * size, size, axis)

    def qkv_piece(layer):
        turned = w_qkv[layer].transpose(1, 2, 0)
        return part_of(turned, out_piece, 1).reshape(3 * out_piece, width)

    def pieces_of(layer):
        return [
            part_of(w_up[layer], hidden_piece, 1).T,
            part_of(w_down[layer], hidden_piece, 0),
            part_of(w_out[layer], out_piece, 0),
            qkv_piece(layer),
        ]

    def rows_of(got, first, count, parts=1):
        rows = got[:, :, first : first + parts * count]
        rows = rows.reshape(n_dp, n_tensor, parts, count, width).transpose(2, 1, 0, 3, 4)
        return lax.optimization_barrier(rows.reshape(parts * n_dp * n_tensor * count, width))

    def weights_of(got):
        if piece % 16 == 0 and hidden_piece == piece and out_piece % 8 == 0:
            return unpack(got, hidden_piece, out_piece)
        up = rows_of(got, 0, hidden_piece)
        down = rows_of(got, hidden_piece, hidden_piece)
        out = rows_of(got, 2 * hidden_piece, out_piece)
        return rows_of(got, 2 * hidden_piece + out_piece, out_piece, 3), up, down, out

    weight_rows = 2 * hidden_piece + 4 * out_piece
    bias_rows = jnp.concatenate([b_qv.reshape(-1), b_up.reshape(-1)])
    bias_rows = jnp.pad(bias_rows, (0, 8 * width - bias_rows.shape[0])).reshape(8, width)
    full = []
    for layer in range(layer_count):
        pieces = pieces_of(layer)
        if layer == 0:
            got = gather(pieces + [bias_rows])
            all_bias = got[0, :, weight_rows:].reshape(n_tensor, 8 * width).astype(f32)
        else:
            pieces, got = lax.optimization_barrier((pieces, got))
            full.append(weights_of(got))
            got = gather(pieces)
    full.append(weights_of(got))

    qv_count = layer_count * 2 * head_cols
    bias_qv = (
        all_bias[:, :qv_count]
        .reshape(n_tensor, layer_count, 2, head_cols)
        .transpose(1, 2, 0, 3)
        .reshape(layer_count, 2, width)
    )
    bias_up = (
        all_bias[:, qv_count : qv_count + layer_count * hidden_cols]
        .reshape(n_tensor, layer_count, hidden_cols)
        .transpose(1, 0, 2)
        .reshape(layer_count, n_tensor * hidden_cols)
    )

    hidden = tokens.astype(f32)
    produced = []
    kept = []
    for layer in range(layer_count):
        normed_one, unit_one, scaled_one = norm_forward(hidden, ln1_gain[layer], ln1_bias[layer])
        normed_one = normed_one.astype(bf16)
        bias = jnp.concatenate([bias_qv[layer, 0], jnp.zeros((width,), f32), bias_qv[layer, 1]])
        full_qkv, full_up, full_down, full_out = full[layer]
        project = (dot_rows(normed_one, full_qkv) + bias).astype(bf16)
        mixed, totals = attention_forward(project, feature_q, feature_k)
        attn = jnp.dot(mixed, full_out, preferred_element_type=f32)
        middle = hidden + keep[layer, 0][:, None] * (attn + b_out[layer].astype(f32))
        normed_two, unit_two, scaled_two = norm_forward(middle, ln2_gain[layer], ln2_bias[layer])
        normed_two = normed_two.astype(bf16)
        upward = dot_rows(normed_two, full_up) + bias_up[layer]
        phi = 0.5 * (1.0 + lax.erf(upward * math.sqrt(0.5)))
        active = (upward * phi).astype(bf16)
        slope = phi + upward * (jnp.exp(-0.5 * upward * upward) * (1.0 / math.sqrt(2 * math.pi)))
        down = jnp.dot(active, full_down, preferred_element_type=f32)
        hidden = middle + keep[layer, 1][:, None] * (down + b_down[layer].astype(f32))
        produced.append(hidden.astype(bf16))
        kept.append(
            (unit_one, scaled_one, normed_one, project, totals, mixed,
             unit_two, scaled_two, normed_two, active, slope)
        )
    blocks_out = jnp.stack(produced)

    def scatter(blocks):
        flat = blocks.reshape((-1,) + blocks.shape[3:])
        flat = flat.reshape(-1, width)
        summed = lax.psum_scatter(flat, groups, scatter_dimension=0, tiled=True)
        return summed.reshape(blocks.shape[2:]).astype(f32)

    grad_flow = cotangent.astype(f32)
    collected = [None] * layer_count
    wide_sums = [None] * layer_count
    narrow_sums = [None] * layer_count
    chains = []
    paired = all(lax.axis_size(axis) & (lax.axis_size(axis) - 1) == 0 for axis in groups)
    for layer in reversed(range(layer_count)):
        (unit_one, scaled_one, normed_one, project, totals, mixed,
         unit_two, scaled_two, normed_two, active, slope) = kept[layer]
        full_qkv, full_up, full_down, full_out = full[layer]
        grad_flow = advance(grad_flow, chains)
        branch_two = keep[layer, 1][:, None] * grad_flow
        grad_bias_down = jnp.sum(branch_two, axis=0)
        branch_two = branch_two.astype(bf16)
        grad_up = dot_rows(branch_two, full_down) * slope
        grad_bias_up = jnp.sum(grad_up, axis=0)
        grad_up = grad_up.astype(bf16)
        wide = (normed_two, grad_up, branch_two, active)
        alone = layer == layer_count - 1 or not paired
        wide = wide_gradients(*wide, (n_dp, n_tensor, 2, piece, width), not alone)
        grad_up, wide = lax.optimization_barrier((grad_up, wide))
        grad_up = advance(grad_up, chains)
        if alone:
            wide_sums[layer] = scatter(wide[0])
        else:
            wide_sums[layer] = [
                PermuteScatter(part[:, :, 0], order)
                for part, order in zip(wide, (rising, turned_about))
            ]
            chains = chains + wide_sums[layer]
        grad_part, grad_gain_two, grad_shift_two = norm_backward(
            jnp.dot(grad_up, full_up, preferred_element_type=f32),
            unit_two, scaled_two, ln2_gain[layer],
        )
        grad_middle = grad_flow + grad_part
        branch_one = keep[layer, 0][:, None] * grad_middle
        grad_bias_out = jnp.sum(branch_one, axis=0)
        branch_one = branch_one.astype(bf16)
        grad_mixed = dot_rows(branch_one, full_out).astype(bf16)
        grad_mixed = advance(grad_mixed, chains)
        *grads, sums = attention_backward(project, feature_q, feature_k, grad_mixed, totals)
        grad_bias_qv = jnp.sum(sums, axis=0)[:2]
        if layer == 0:
            wide_sums[-1], *grads = lax.optimization_barrier((wide_sums[-1], *grads))
        grads = advance(grads, chains)
        (narrow,) = narrow_gradients(
            normed_one, grads, branch_one, mixed, (n_dp, n_tensor, 1, piece, width)
        )
        grads, narrow = lax.optimization_barrier((grads, narrow))
        if layer == 0 or not paired:
            narrow_sums[layer] = scatter(narrow)[0]
        else:
            narrow_sums[layer] = PermuteScatter(narrow[:, :, 0], rising)
            chains = chains + [narrow_sums[layer]]
        grad_one = sum(
            jnp.dot(
                grads[part],
                full_qkv[part * width : (part + 1) * width],
                preferred_element_type=f32,
            )
            for part in range(3)
        )
        grad_part, grad_gain_one, grad_shift_one = norm_backward(
            grad_one, unit_one, scaled_one, ln1_gain[layer]
        )
        grad_flow = grad_middle + grad_part
        collected[layer] = jnp.concatenate(
            [grad_gain_one, grad_shift_one, grad_bias_qv.reshape(-1), grad_bias_out,
             grad_gain_two, grad_shift_two, grad_bias_down, grad_bias_up]
        )
    small = jnp.stack(collected)
    for axis in groups:
        small = sum_over(small, axis, lax.axis_size(axis))
    grad_qkv, grad_out, grad_up, grad_down = [], [], [], []
    for layer in range(layer_count):
        narrow = narrow_sums[layer]
        if isinstance(narrow, PermuteScatter):
            narrow = narrow.finish()
        wide = [
            part.finish() if isinstance(part, PermuteScatter) else part
            for part in wide_sums[layer]
        ]
        grad_qkv.append(narrow[:, : 3 * head_cols].reshape(piece, 3, head_cols))
        grad_out.append(narrow[:, 3 * head_cols :].T)
        grad_up.append(wide[0])
        grad_down.append(wide[1].T)
    grad_qkv, grad_out, grad_up, grad_down = [
        jnp.stack(parts) for parts in (grad_qkv, grad_out, grad_up, grad_down)
    ]
    gain_one, shift_one, query_bias, value_bias, bias_out, gain_two, shift_two, bias_down = [
        small[:, position * width : (position + 1) * width] for position in range(8)
    ]
    return (
        blocks_out,
        grad_flow,
        gain_one,
        shift_one,
        grad_qkv,
        jnp.stack([query_bias, value_bias], axis=1),
        grad_out,
        bias_out,
        gain_two,
        shift_two,
        grad_up,
        small[:, 8 * width :],
        grad_down,
        bias_down,
    )


def solution(mesh):
    in_specs = (
        P(("dp", "tensor"), None),
        P(("dp", "tensor"), None),
        P("dp", None),
        P(None, None, "dp", None),
        P(),
        P(),
        P(None, None, None, "tensor"),
        P(None, None, "tensor"),
        P(None, "tensor", None),
        P(),
        P(),
        P(),
        P(None, None, "tensor"),
        P(None, "tensor"),
        P(None, "tensor", None),
        P(),
    )
    out_specs = (
        P(None, ("dp", "tensor"), None),
        P(("dp", "tensor"), None),
        P(),
        P(),
        P(None, "dp", None, "tensor"),
        P(),
        P(None, "tensor", "dp"),
        P(),
        P(),
        P(),
        P(None, "dp", "tensor"),
        P(),
        P(None, "tensor", "dp"),
        P(),
    )
    return jax.shard_map(
        per_device, mesh=mesh, in_specs=in_specs, out_specs=out_specs, check_vma=False
    )
```

```python
import math

import jax
import jax.numpy as jnp
from jax import lax
from jax.experimental import pallas as pl
from jax.experimental.pallas import tpu as pltpu
from jax.sharding import PartitionSpec as P

HEAD_DIM = 64
SEQ = 1024
MOST_LEN = 256
PAIR = 2 * HEAD_DIM

eps_norm = 1e-06
survival = 0.9
masked_score = -1e30
score_scale = 1.0 / math.sqrt(HEAD_DIM)
groups = ("dp", "tensor")
bf16 = jnp.bfloat16
f32 = jnp.float32


def norm_forward(values, norm_gain, norm_shift):
    centre = values - jnp.mean(values, axis=-1, keepdims=True)
    spread = jnp.mean(centre * centre, axis=-1, keepdims=True)
    scaled = lax.rsqrt(spread + eps_norm)
    normalized = centre * scaled
    return (normalized * norm_gain + norm_shift, normalized, scaled)


def norm_backward(grad_out, normalized, scaled, norm_gain):
    grad_unit = grad_out * norm_gain
    inner = (
        grad_unit
        - jnp.mean(grad_unit, axis=-1, keepdims=True)
        - normalized * jnp.mean(grad_unit * normalized, axis=-1, keepdims=True)
    )
    return (inner * scaled, jnp.sum(grad_out * normalized, axis=0), jnp.sum(grad_out, axis=0))


def key_window(block):
    return max(0, (block - 1) * MOST_LEN), min(SEQ, (block + 2) * MOST_LEN)


def own_lanes(head):
    lane = lax.broadcasted_iota(jnp.int32, (1, PAIR), 1)
    return lane < HEAD_DIM if head == 0 else lane >= HEAD_DIM


def dot_rows(left, right):
    return lax.dot_general(left, right, (((1,), (1,)), ((), ())), preferred_element_type=f32)


def dot_tokens(left, right):
    return lax.dot_general(left, right, (((0,), (0,)), ((), ())), preferred_element_type=f32)


def attention_forward_kernel(q_ref, k_ref, v_ref, fq_ref, fk_ref, mixed_ref, total_ref):
    for block in range(SEQ // MOST_LEN):
        rows = slice(block * MOST_LEN, (block + 1) * MOST_LEN)
        keys = slice(*key_window(block))
        mixed = []
        totals = []
        for head in (0, 1):
            own = own_lanes(head)
            query = jnp.where(own, q_ref[rows, :] * bf16(score_scale), fq_ref[rows, :])
            key = jnp.where(own, k_ref[keys, :], fk_ref[keys, :])
            scores = dot_rows(query, key)
            top = jnp.max(scores, axis=-1, keepdims=True)
            exponent = jnp.exp(scores - top)
            total = jnp.sum(exponent, axis=-1, keepdims=True)
            part = jnp.dot(exponent.astype(bf16), v_ref[keys, :], preferred_element_type=f32)
            mixed.append(part / total)
            totals.append(top + jnp.log(total))
        own = own_lanes(0)
        mixed_ref[rows, :] = jnp.where(own, mixed[0], mixed[1]).astype(bf16)
        total_ref[rows, :] = jnp.where(own, totals[0], totals[1])


def attention_backward_kernel(
    q_ref, k_ref, v_ref, fq_ref, fk_ref, grad_ref, total_ref,
    dq_ref, dk_ref, dv_ref, sums_ref, dk_acc, dv_acc,
):
    dk_acc[...] = jnp.zeros_like(dk_acc)
    dv_acc[...] = jnp.zeros_like(dv_acc)
    query_sum = jnp.zeros((1, PAIR), f32)
    for block in range(SEQ // MOST_LEN):
        rows = slice(block * MOST_LEN, (block + 1) * MOST_LEN)
        keys = slice(*key_window(block))
        grad_query = jnp.zeros((MOST_LEN, PAIR), f32)
        for head in (0, 1):
            own = own_lanes(head)
            scaled = q_ref[rows, :] * bf16(score_scale)
            query = jnp.where(own, scaled, fq_ref[rows, :])
            key = jnp.where(own, k_ref[keys, :], fk_ref[keys, :])
            scores = dot_rows(query, key)
            lane = head * HEAD_DIM
            weights = jnp.exp(scores - total_ref[rows, lane : lane + 1])
            zero = jnp.zeros((), bf16)
            grad = jnp.where(own, grad_ref[rows, :], zero)
            product = weights * dot_rows(grad, v_ref[keys, :])
            inner = jnp.sum(product, axis=-1, keepdims=True)
            grad_scores = (product - weights * inner).astype(bf16)
            grad_query += jnp.dot(
                grad_scores, jnp.where(own, k_ref[keys, :], zero), preferred_element_type=f32
            )
            dk_acc[keys, :] += dot_tokens(grad_scores, jnp.where(own, scaled, zero))
            dv_acc[keys, :] += dot_tokens(weights.astype(bf16), grad)
        grad_query *= score_scale
        query_sum += jnp.sum(grad_query, axis=0, keepdims=True)
        dq_ref[rows, :] = grad_query.astype(bf16)
    dk_ref[...] = dk_acc[...].astype(bf16)
    dv_ref[...] = dv_acc[...].astype(bf16)
    value_sum = jnp.sum(dv_acc[...], axis=0, keepdims=True)
    row = lax.broadcasted_iota(jnp.int32, (8, PAIR), 0)
    sums_ref[0, :, :] = jnp.where(row == 0, query_sum, value_sum)


def attention_specs(pairs):
    def part(index):
        return pl.BlockSpec((SEQ, PAIR), lambda r, p: (r, index * pairs + p))

    feature = pl.BlockSpec((SEQ, PAIR), lambda r, p: (r, 0))
    own = pl.BlockSpec((SEQ, PAIR), lambda r, p: (r, p))
    return [part(0), part(1), part(2), feature, feature], own


def attention_forward(project, feature_q, feature_k):
    tokens, width = project.shape[0], project.shape[1] // 3
    pairs = width // PAIR
    ins, own = attention_specs(pairs)
    return pl.pallas_call(
        attention_forward_kernel,
        grid=(tokens // SEQ, pairs),
        in_specs=ins,
        out_specs=[own, own],
        out_shape=[
            jax.ShapeDtypeStruct((tokens, width), bf16),
            jax.ShapeDtypeStruct((tokens, width), f32),
        ],
        cost_estimate=pl.CostEstimate(
            flops=4 * tokens * 3 * MOST_LEN * 2 * width,
            bytes_accessed=tokens * width * 12,
            transcendentals=tokens * 3 * MOST_LEN * width // HEAD_DIM,
        ),
        compiler_params=pltpu.CompilerParams(vmem_limit_bytes=48 << 20),
        name="attend",
    )(project, project, project, feature_q, feature_k)


def attention_backward(project, feature_q, feature_k, grad_mixed, totals):
    tokens, width = grad_mixed.shape
    pairs = width // PAIR
    ins, own = attention_specs(pairs)
    low = jax.ShapeDtypeStruct((tokens, width), bf16)
    return pl.pallas_call(
        attention_backward_kernel,
        grid=(tokens // SEQ, pairs),
        in_specs=ins + [own, own],
        out_specs=[own, own, own, pl.BlockSpec((1, 8, PAIR), lambda r, p: (r, 0, p))],
        out_shape=[low, low, low, jax.ShapeDtypeStruct((tokens // SEQ, 8, width), f32)],
        scratch_shapes=[pltpu.VMEM((SEQ, PAIR), f32), pltpu.VMEM((SEQ, PAIR), f32)],
        cost_estimate=pl.CostEstimate(
            flops=10 * tokens * 3 * MOST_LEN * 2 * width,
            bytes_accessed=tokens * width * 18,
            transcendentals=tokens * 3 * MOST_LEN * width // HEAD_DIM,
        ),
        compiler_params=pltpu.CompilerParams(vmem_limit_bytes=48 << 20),
        name="attend_back",
    )(project, project, project, feature_q, feature_k, grad_mixed, totals)


def unpack_kernel(got_ref, qkv_ref, up_ref, down_ref, out_ref):
    blocks, hidden, few = up_ref.shape[1], up_ref.shape[2], out_ref.shape[2]
    for block in range(blocks):
        up_ref[0, block] = got_ref[block, 0, :hidden, :]
        down_ref[0, block] = got_ref[block, 0, hidden : 2 * hidden, :]
        out_ref[0, block] = got_ref[block, 0, 2 * hidden : 2 * hidden + few, :]
        for part in range(3):
            first = 2 * hidden + (1 + part) * few
            qkv_ref[part, 0, block] = got_ref[block, 0, first : first + few, :]


def unpack(got, hidden, few):
    n_dp, n_tensor, rows, width = got.shape

    def spec(count):
        return pl.BlockSpec((1, n_dp, count, width), lambda t: (t, 0, 0, 0))

    def shape(count):
        return jax.ShapeDtypeStruct((n_tensor, n_dp, count, width), bf16)

    outs = pl.pallas_call(
        unpack_kernel,
        grid=(n_tensor,),
        in_specs=[pl.BlockSpec((n_dp, 1, rows, width), lambda t: (0, t, 0, 0))],
        out_specs=[
            pl.BlockSpec((3, 1, n_dp, few, width), lambda t: (0, t, 0, 0, 0)),
            spec(hidden),
            spec(hidden),
            spec(few),
        ],
        out_shape=[
            jax.ShapeDtypeStruct((3, n_tensor, n_dp, few, width), bf16),
            shape(hidden),
            shape(hidden),
            shape(few),
        ],
        cost_estimate=pl.CostEstimate(
            flops=0, bytes_accessed=4 * n_dp * n_tensor * rows * width, transcendentals=0
        ),
        compiler_params=pltpu.CompilerParams(vmem_limit_bytes=48 << 20),
        name="unpack",
    )(got)
    return [array.reshape(-1, width) for array in outs]


class PermuteSum:
    def __init__(self, blocks):
        sizes = {axis: lax.axis_size(axis) for axis in groups}
        self.blocks = blocks
        self.steps = [
            (axis, bit) for axis in groups for bit in range(sizes[axis].bit_length() - 1)
        ]

    def step(self):
        axis, bit = self.steps.pop(0)
        pairs = [(index, index ^ (1 << bit)) for index in range(lax.axis_size(axis))]
        self.blocks = self.blocks + lax.ppermute(self.blocks, axis, pairs)


class PermuteScatter:
    def __init__(self, blocks, order):
        self.bits = {axis: lax.axis_size(axis).bit_length() - 1 for axis in groups}
        self.left = [(axis, bit) for axis in groups for bit in reversed(range(self.bits[axis]))]
        self.blocks = blocks.reshape((2,) * len(self.left) + blocks.shape[2:])
        self.steps = order(self.bits)

    def step(self):
        axis, bit = self.steps.pop(0)
        dim = self.left.index((axis, bit))
        self.left.pop(dim)
        side = (lax.axis_index(axis) >> bit) & 1
        sent = lax.dynamic_index_in_dim(self.blocks, 1 - side, dim, keepdims=False)
        own = lax.dynamic_index_in_dim(self.blocks, side, dim, keepdims=False)
        pairs = [(index, index ^ (1 << bit)) for index in range(1 << self.bits[axis])]
        blocks = own.astype(f32) + lax.ppermute(sent, axis, pairs).astype(f32)
        self.blocks = blocks.astype(bf16) if self.left else blocks


def tie(value, chains):
    value, blocks = lax.optimization_barrier((value, [chain.blocks for chain in chains]))
    for chain, block in zip(chains, blocks):
        chain.blocks = block
    return value


def advance(value, chains):
    chains = [chain for chain in chains if chain.steps]
    for chain in chains:
        chain.step()
    return tie(value, chains)


def rising(bits):
    return [(axis, bit) for axis in groups for bit in range(bits[axis])]


def turned_about(bits):
    steps = rising(bits)
    count = bits[groups[0]]
    return steps[:1] + steps[1:count][::-1] + steps[count:]


def wide_kernel(norm_ref, up_ref, branch_ref, active_ref, *rest):
    *out_refs, turned, result = rest
    piece = out_refs[0].shape[3]
    step = pl.program_id(0)
    for position, (left_ref, right_ref) in enumerate(
        ((norm_ref, up_ref), (branch_ref, active_ref))
    ):
        out_ref = out_refs[position % len(out_refs)]

        @pl.when(step == position)
        def _():
            @pl.when(pl.program_id(1) == 0)
            def _():
                turned[...] = left_ref[...].T

            result[...] = jnp.dot(turned[...], right_ref[...], preferred_element_type=f32)
            for block in range(out_ref.shape[0]):
                out_ref[block, 0, 0] = result[block * piece : (block + 1) * piece, :].astype(bf16)


def narrow_kernel(
    norm_ref, dq_ref, dk_ref, dv_ref, branch_ref, mixed_ref,
    out_ref, turned, result,
):
    blocks, shards, _, piece, columns = out_ref.shape
    columns //= 4
    for position, right_ref in enumerate((dq_ref, dk_ref, dv_ref, mixed_ref)):
        if position == 0:
            turned[...] = norm_ref[...].T
        if position == 3:
            turned[...] = branch_ref[...].T
        result[...] = jnp.dot(turned[...], right_ref[...], preferred_element_type=f32)
        for block in range(blocks):
            for shard in range(shards):
                out_ref[block, shard, 0, :, position * columns : (position + 1) * columns] = (
                    result[
                        block * piece : (block + 1) * piece,
                        shard * columns : (shard + 1) * columns,
                    ].astype(bf16)
                )


def blocked_gradients(kernel, ins, in_specs, grid, out_spec, shape, products, name):
    tokens, width = ins[0].shape
    return pl.pallas_call(
        kernel,
        grid=grid,
        in_specs=in_specs,
        out_specs=out_spec,
        out_shape=[jax.ShapeDtypeStruct(shape, bf16)] * len(out_spec),
        scratch_shapes=[pltpu.VMEM((width, tokens), bf16), pltpu.VMEM((width, width), f32)],
        cost_estimate=pl.CostEstimate(
            flops=2 * products * tokens * width * width,
            bytes_accessed=products * 2 * (tokens * width + width * width),
            transcendentals=0,
        ),
        compiler_params=pltpu.CompilerParams(vmem_limit_bytes=56 << 20),
        name=name,
    )(*ins)


def wide_gradients(normed, grad_up, branch, active, shape, split):
    tokens, width = normed.shape
    n_dp, n_tensor, _, piece, _ = shape
    whole = pl.BlockSpec((tokens, width), lambda s, t: (0, 0))
    last = n_tensor - 1
    if split:
        indices = [
            lambda s, t: (0, jnp.where(s == 0, t, last), 0, 0, 0),
            lambda s, t: (0, jnp.where(s == 1, t, 0), 0, 0, 0),
        ]
    else:
        indices = [lambda s, t: (0, t, s, 0, 0)]
    return blocked_gradients(
        wide_kernel,
        [normed, grad_up, branch, active],
        [
            whole,
            pl.BlockSpec((tokens, width), lambda s, t: (0, jnp.where(s == 0, t, last))),
            whole,
            pl.BlockSpec((tokens, width), lambda s, t: (0, jnp.where(s == 1, t, 0))),
        ],
        (2, n_tensor),
        [pl.BlockSpec((n_dp, 1, 1, piece, width), index) for index in indices],
        shape[:2] + (1 if split else 2,) + shape[3:],
        2 * n_tensor,
        "wide_grads",
    )


def narrow_gradients(normed, grads, branch, mixed, shape):
    tokens, width = normed.shape
    n_dp, n_tensor, _, piece, _ = shape
    whole = pl.BlockSpec((tokens, width), lambda s: (0, 0))
    return blocked_gradients(
        narrow_kernel,
        [normed, *grads, branch, mixed],
        [whole] * 6,
        (1,),
        [pl.BlockSpec((n_dp, n_tensor, 1, piece, width), lambda s: (0, 0, 0, 0, 0))],
        shape,
        4,
        "narrow_grads",
    )


def per_device(
    tokens,
    cotangent,
    lengths,
    drop_mask,
    ln1_gain,
    ln1_bias,
    w_qkv,
    b_qv,
    w_out,
    b_out,
    ln2_gain,
    ln2_bias,
    w_up,
    b_up,
    w_down,
    b_down,
):
    layer_count = w_qkv.shape[0]
    local_rows, width = tokens.shape
    segment_count = lengths.shape[1]
    tensor_index = lax.axis_index("tensor")
    dp_index = lax.axis_index("dp")
    n_dp = lax.axis_size("dp")
    n_tensor = lax.axis_size("tensor")
    own_rows = local_rows // SEQ
    head_cols = w_qkv.shape[3]
    hidden_cols = w_up.shape[2]
    piece = width // n_dp
    out_piece = head_cols // n_dp
    hidden_piece = hidden_cols // n_dp

    own_lengths = lax.dynamic_slice_in_dim(lengths, tensor_index * own_rows, own_rows, 0)
    own_mask = lax.dynamic_slice_in_dim(drop_mask, tensor_index * own_rows, own_rows, 2)
    segment_ends = jnp.cumsum(own_lengths, axis=-1)
    positions = jnp.arange(SEQ, dtype=jnp.int32)
    segments = jnp.sum(
        (positions[None, :, None] >= segment_ends[:, None, :]).astype(jnp.int32), axis=-1
    )
    onehot = (
        segments[:, :, None] == jnp.arange(segment_count, dtype=jnp.int32)[None, None, :]
    ).astype(f32)
    keep = (
        jnp.sum(onehot[None, None] * own_mask.astype(f32)[:, :, :, None, :], axis=-1) / survival
    ).reshape(layer_count, 2, local_rows)
    lane = jnp.arange(PAIR, dtype=jnp.int32)[None, :] % HEAD_DIM
    same = segments.reshape(local_rows, 1) == lane
    feature_q = same.astype(bf16)
    feature_k = jnp.where(same | (lane >= segment_count), 0.0, masked_score).astype(bf16)

    def gather(pieces):
        rows = jnp.concatenate(pieces, axis=0)
        gathered = lax.all_gather(rows, groups, axis=0, tiled=False)
        return gathered.reshape((n_dp, n_tensor) + rows.shape)

    def part_of(array, size, axis):
        return lax.dynamic_slice_in_dim(array, dp_index * size, size, axis)

    def qkv_piece(layer):
        turned = w_qkv[layer].transpose(1, 2, 0)
        return part_of(turned, out_piece, 1).reshape(3 * out_piece, width)

    def pieces_of(layer):
        return [
            part_of(w_up[layer], hidden_piece, 1).T,
            part_of(w_down[layer], hidden_piece, 0),
            part_of(w_out[layer], out_piece, 0),
            qkv_piece(layer),
        ]

    def rows_of(got, first, count, parts=1):
        rows = got[:, :, first : first + parts * count]
        rows = rows.reshape(n_dp, n_tensor, parts, count, width).transpose(2, 1, 0, 3, 4)
        return lax.optimization_barrier(rows.reshape(parts * n_dp * n_tensor * count, width))

    def weights_of(got):
        if piece % 16 == 0 and hidden_piece == piece and out_piece % 8 == 0:
            return unpack(got, hidden_piece, out_piece)
        up = rows_of(got, 0, hidden_piece)
        down = rows_of(got, hidden_piece, hidden_piece)
        out = rows_of(got, 2 * hidden_piece, out_piece)
        return rows_of(got, 2 * hidden_piece + out_piece, out_piece, 3), up, down, out

    weight_rows = 2 * hidden_piece + 4 * out_piece
    bias_rows = jnp.concatenate([b_qv.reshape(-1), b_up.reshape(-1)])
    bias_rows = jnp.pad(bias_rows, (0, 8 * width - bias_rows.shape[0])).reshape(8, width)
    full = []
    hidden = tokens.astype(f32)
    early = (norm_forward(hidden, ln1_gain[0], ln1_bias[0]), feature_q, feature_k, keep)
    for layer in range(layer_count):
        pieces = pieces_of(layer)
        if layer == 0:
            got = gather(pieces + [bias_rows])
            all_bias = got[0, :, weight_rows:].reshape(n_tensor, 8 * width).astype(f32)
        else:
            pieces, got, early = lax.optimization_barrier((pieces, got, early))
            full.append(weights_of(got))
            got = gather(pieces)
    full.append(weights_of(got))

    qv_count = layer_count * 2 * head_cols
    bias_qv = (
        all_bias[:, :qv_count]
        .reshape(n_tensor, layer_count, 2, head_cols)
        .transpose(1, 2, 0, 3)
        .reshape(layer_count, 2, width)
    )
    bias_up = (
        all_bias[:, qv_count : qv_count + layer_count * hidden_cols]
        .reshape(n_tensor, layer_count, hidden_cols)
        .transpose(1, 0, 2)
        .reshape(layer_count, n_tensor * hidden_cols)
    )

    first_norm, feature_q, feature_k, keep = early
    produced = []
    kept = []
    for layer in range(layer_count):
        if layer > 0:
            first_norm = norm_forward(hidden, ln1_gain[layer], ln1_bias[layer])
        normed_one, unit_one, scaled_one = first_norm
        normed_one = normed_one.astype(bf16)
        bias = jnp.concatenate([bias_qv[layer, 0], jnp.zeros((width,), f32), bias_qv[layer, 1]])
        full_qkv, full_up, full_down, full_out = full[layer]
        project = (dot_rows(normed_one, full_qkv) + bias).astype(bf16)
        mixed, totals = attention_forward(project, feature_q, feature_k)
        attn = jnp.dot(mixed, full_out, preferred_element_type=f32)
        middle = hidden + keep[layer, 0][:, None] * (attn + b_out[layer].astype(f32))
        normed_two, unit_two, scaled_two = norm_forward(middle, ln2_gain[layer], ln2_bias[layer])
        normed_two = normed_two.astype(bf16)
        upward = dot_rows(normed_two, full_up) + bias_up[layer]
        phi = 0.5 * (1.0 + lax.erf(upward * math.sqrt(0.5)))
        active = (upward * phi).astype(bf16)
        slope = phi + upward * (jnp.exp(-0.5 * upward * upward) * (1.0 / math.sqrt(2 * math.pi)))
        down = jnp.dot(active, full_down, preferred_element_type=f32)
        hidden = middle + keep[layer, 1][:, None] * (down + b_down[layer].astype(f32))
        produced.append(hidden.astype(bf16))
        kept.append(
            (unit_one, scaled_one, normed_one, project, totals, mixed,
             unit_two, scaled_two, normed_two, active, slope)
        )
    blocks_out = jnp.stack(produced)

    def scatter(blocks):
        flat = blocks.reshape((-1,) + blocks.shape[3:])
        flat = flat.reshape(-1, width)
        summed = lax.psum_scatter(flat, groups, scatter_dimension=0, tiled=True)
        return summed.reshape(blocks.shape[2:]).astype(f32)

    grad_flow = cotangent.astype(f32)
    collected = [None] * layer_count
    wide_sums = [None] * layer_count
    narrow_sums = [None] * layer_count
    chains = []
    paired = all(lax.axis_size(axis) & (lax.axis_size(axis) - 1) == 0 for axis in groups)
    for layer in reversed(range(layer_count)):
        (unit_one, scaled_one, normed_one, project, totals, mixed,
         unit_two, scaled_two, normed_two, active, slope) = kept[layer]
        full_qkv, full_up, full_down, full_out = full[layer]
        grad_flow = advance(grad_flow, chains)
        branch_two = keep[layer, 1][:, None] * grad_flow
        grad_bias_down = jnp.sum(branch_two, axis=0)
        branch_two = branch_two.astype(bf16)
        grad_up = dot_rows(branch_two, full_down) * slope
        grad_bias_up = jnp.sum(grad_up, axis=0)
        grad_up = grad_up.astype(bf16)
        wide = (normed_two, grad_up, branch_two, active)
        alone = layer == layer_count - 1 or not paired
        wide = wide_gradients(*wide, (n_dp, n_tensor, 2, piece, width), not alone)
        grad_up, wide = lax.optimization_barrier((grad_up, wide))
        grad_up = advance(grad_up, chains)
        if alone:
            wide_sums[layer] = scatter(wide[0])
        else:
            wide_sums[layer] = [
                PermuteScatter(part[:, :, 0], order)
                for part, order in zip(wide, (rising, turned_about))
            ]
            chains = chains + wide_sums[layer]
        grad_part, grad_gain_two, grad_shift_two = norm_backward(
            jnp.dot(grad_up, full_up, preferred_element_type=f32),
            unit_two, scaled_two, ln2_gain[layer],
        )
        grad_middle = grad_flow + grad_part
        branch_one = keep[layer, 0][:, None] * grad_middle
        grad_bias_out = jnp.sum(branch_one, axis=0)
        branch_one = branch_one.astype(bf16)
        grad_mixed = dot_rows(branch_one, full_out).astype(bf16)
        grad_mixed = advance(grad_mixed, chains)
        *grads, sums = attention_backward(project, feature_q, feature_k, grad_mixed, totals)
        grad_bias_qv = jnp.sum(sums, axis=0)[:2]
        if layer == 0:
            wide_sums[-1], *grads = lax.optimization_barrier((wide_sums[-1], *grads))
        grads = advance(grads, chains)
        (narrow,) = narrow_gradients(
            normed_one, grads, branch_one, mixed, (n_dp, n_tensor, 1, piece, width)
        )
        grads, narrow = lax.optimization_barrier((grads, narrow))
        if not paired:
            narrow_sums[layer] = [scatter(narrow)[0]]
        elif layer == 0 and piece % 2 == 0:
            narrow_sums[layer] = [
                PermuteScatter(part, order)
                for part, order in zip(
                    jnp.split(narrow[:, :, 0], 2, axis=2), (rising, turned_about)
                )
            ]
        else:
            narrow_sums[layer] = [PermuteScatter(narrow[:, :, 0], rising)]
        if paired:
            chains = chains + narrow_sums[layer]
        grad_one = sum(
            jnp.dot(
                grads[part],
                full_qkv[part * width : (part + 1) * width],
                preferred_element_type=f32,
            )
            for part in range(3)
        )
        grad_part, grad_gain_one, grad_shift_one = norm_backward(
            grad_one, unit_one, scaled_one, ln1_gain[layer]
        )
        grad_flow = grad_middle + grad_part
        collected[layer] = [
            grad_gain_one, grad_shift_one, grad_bias_qv[0], grad_bias_qv[1], grad_bias_out,
            grad_gain_two, grad_shift_two, grad_bias_down,
            *grad_bias_up.reshape(-1, width),
        ]
    small = jnp.stack([row for rows in collected for row in rows])
    if paired:
        small = PermuteSum(advance(small, chains))
        chains = chains + [small]
        while any(chain.steps for chain in chains):
            advance((), chains)
        small = small.blocks
    else:
        small = lax.psum(small, groups)
    grad_qkv, grad_out, grad_up, grad_down = [], [], [], []
    for layer in range(layer_count):
        narrow, wide = [
            [part.blocks if isinstance(part, PermuteScatter) else part for part in sums[layer]]
            for sums in (narrow_sums, wide_sums)
        ]
        narrow = jnp.concatenate(narrow, axis=0)
        grad_qkv.append(narrow[:, : 3 * head_cols].reshape(piece, 3, head_cols))
        grad_out.append(narrow[:, 3 * head_cols :].T)
        grad_up.append(wide[0])
        grad_down.append(wide[1].T)
    grad_qkv, grad_out, grad_up, grad_down = [
        jnp.stack(parts) for parts in (grad_qkv, grad_out, grad_up, grad_down)
    ]
    small = small.reshape(layer_count, -1)
    gain_one, shift_one, query_bias, value_bias, bias_out, gain_two, shift_two, bias_down = [
        small[:, position * width : (position + 1) * width] for position in range(8)
    ]
    return (
        blocks_out,
        grad_flow,
        gain_one,
        shift_one,
        grad_qkv,
        jnp.stack([query_bias, value_bias], axis=1),
        grad_out,
        bias_out,
        gain_two,
        shift_two,
        grad_up,
        small[:, 8 * width :],
        grad_down,
        bias_down,
    )


def solution(mesh):
    in_specs = (
        P(("dp", "tensor"), None),
        P(("dp", "tensor"), None),
        P("dp", None),
        P(None, None, "dp", None),
        P(),
        P(),
        P(None, None, None, "tensor"),
        P(None, None, "tensor"),
        P(None, "tensor", None),
        P(),
        P(),
        P(),
        P(None, None, "tensor"),
        P(None, "tensor"),
        P(None, "tensor", None),
        P(),
    )
    out_specs = (
        P(None, ("dp", "tensor"), None),
        P(("dp", "tensor"), None),
        P(),
        P(),
        P(None, "dp", None, "tensor"),
        P(),
        P(None, "tensor", "dp"),
        P(),
        P(),
        P(),
        P(None, "dp", "tensor"),
        P(),
        P(None, "tensor", "dp"),
        P(),
    )
    return jax.shard_map(
        per_device, mesh=mesh, in_specs=in_specs, out_specs=out_specs, check_vma=False
    )
```

```python
import math

import jax
import jax.numpy as jnp
from jax import lax
from jax.experimental import pallas as pl
from jax.experimental.pallas import tpu as pltpu
from jax.sharding import PartitionSpec as P

HEAD_DIM = 64
SEQ = 1024
MOST_LEN = 256
PAIR = 2 * HEAD_DIM

eps_norm = 1e-06
survival = 0.9
masked_score = -1e30
score_scale = 1.0 / math.sqrt(HEAD_DIM)
groups = ("dp", "tensor")
bf16 = jnp.bfloat16
f32 = jnp.float32


def norm_forward(values, norm_gain, norm_shift):
    centre = values - jnp.mean(values, axis=-1, keepdims=True)
    spread = jnp.mean(centre * centre, axis=-1, keepdims=True)
    scaled = lax.rsqrt(spread + eps_norm)
    normalized = centre * scaled
    return (normalized * norm_gain + norm_shift, normalized, scaled)


def norm_backward(grad_out, normalized, scaled, norm_gain):
    grad_unit = grad_out * norm_gain
    inner = (
        grad_unit
        - jnp.mean(grad_unit, axis=-1, keepdims=True)
        - normalized * jnp.mean(grad_unit * normalized, axis=-1, keepdims=True)
    )
    return (inner * scaled, jnp.sum(grad_out * normalized, axis=0), jnp.sum(grad_out, axis=0))


def key_window(block):
    return max(0, (block - 1) * MOST_LEN), min(SEQ, (block + 2) * MOST_LEN)


def own_lanes(head):
    lane = lax.broadcasted_iota(jnp.int32, (1, PAIR), 1)
    return lane < HEAD_DIM if head == 0 else lane >= HEAD_DIM


def dot_rows(left, right):
    return lax.dot_general(left, right, (((1,), (1,)), ((), ())), preferred_element_type=f32)


def dot_tokens(left, right):
    return lax.dot_general(left, right, (((0,), (0,)), ((), ())), preferred_element_type=f32)


def attention_forward_kernel(q_ref, k_ref, v_ref, fq_ref, fk_ref, mixed_ref, total_ref):
    for block in range(SEQ // MOST_LEN):
        rows = slice(block * MOST_LEN, (block + 1) * MOST_LEN)
        keys = slice(*key_window(block))
        mixed = []
        totals = []
        for head in (0, 1):
            own = own_lanes(head)
            query = jnp.where(own, q_ref[rows, :] * bf16(score_scale), fq_ref[rows, :])
            key = jnp.where(own, k_ref[keys, :], fk_ref[keys, :])
            scores = dot_rows(query, key)
            top = jnp.max(scores, axis=-1, keepdims=True)
            exponent = jnp.exp(scores - top)
            total = jnp.sum(exponent, axis=-1, keepdims=True)
            part = jnp.dot(exponent.astype(bf16), v_ref[keys, :], preferred_element_type=f32)
            mixed.append(part / total)
            totals.append(top + jnp.log(total))
        own = own_lanes(0)
        mixed_ref[rows, :] = jnp.where(own, mixed[0], mixed[1]).astype(bf16)
        total_ref[rows, :] = jnp.where(own, totals[0], totals[1])


def attention_backward_kernel(
    q_ref, k_ref, v_ref, fq_ref, fk_ref, grad_ref, total_ref,
    dq_ref, dk_ref, dv_ref, sums_ref, dk_acc, dv_acc,
):
    dk_acc[...] = jnp.zeros_like(dk_acc)
    dv_acc[...] = jnp.zeros_like(dv_acc)
    query_sum = jnp.zeros((1, PAIR), f32)
    for block in range(SEQ // MOST_LEN):
        rows = slice(block * MOST_LEN, (block + 1) * MOST_LEN)
        keys = slice(*key_window(block))
        grad_query = jnp.zeros((MOST_LEN, PAIR), f32)
        for head in (0, 1):
            own = own_lanes(head)
            scaled = q_ref[rows, :] * bf16(score_scale)
            query = jnp.where(own, scaled, fq_ref[rows, :])
            key = jnp.where(own, k_ref[keys, :], fk_ref[keys, :])
            scores = dot_rows(query, key)
            lane = head * HEAD_DIM
            weights = jnp.exp(scores - total_ref[rows, lane : lane + 1])
            zero = jnp.zeros((), bf16)
            grad = jnp.where(own, grad_ref[rows, :], zero)
            product = weights * dot_rows(grad, v_ref[keys, :])
            inner = jnp.sum(product, axis=-1, keepdims=True)
            grad_scores = (product - weights * inner).astype(bf16)
            grad_query += jnp.dot(
                grad_scores, jnp.where(own, k_ref[keys, :], zero), preferred_element_type=f32
            )
            dk_acc[keys, :] += dot_tokens(grad_scores, jnp.where(own, scaled, zero))
            dv_acc[keys, :] += dot_tokens(weights.astype(bf16), grad)
        grad_query *= score_scale
        query_sum += jnp.sum(grad_query, axis=0, keepdims=True)
        dq_ref[rows, :] = grad_query.astype(bf16)
    dk_ref[...] = dk_acc[...].astype(bf16)
    dv_ref[...] = dv_acc[...].astype(bf16)
    value_sum = jnp.sum(dv_acc[...], axis=0, keepdims=True)
    row = lax.broadcasted_iota(jnp.int32, (8, PAIR), 0)
    sums_ref[0, :, :] = jnp.where(row == 0, query_sum, value_sum)


def attention_specs(pairs):
    def part(index):
        return pl.BlockSpec((SEQ, PAIR), lambda r, p: (r, index * pairs + p))

    feature = pl.BlockSpec((SEQ, PAIR), lambda r, p: (r, 0))
    own = pl.BlockSpec((SEQ, PAIR), lambda r, p: (r, p))
    return [part(0), part(1), part(2), feature, feature], own


def attention_forward(project, feature_q, feature_k):
    tokens, width = project.shape[0], project.shape[1] // 3
    pairs = width // PAIR
    ins, own = attention_specs(pairs)
    return pl.pallas_call(
        attention_forward_kernel,
        grid=(tokens // SEQ, pairs),
        in_specs=ins,
        out_specs=[own, own],
        out_shape=[
            jax.ShapeDtypeStruct((tokens, width), bf16),
            jax.ShapeDtypeStruct((tokens, width), f32),
        ],
        cost_estimate=pl.CostEstimate(
            flops=4 * tokens * 3 * MOST_LEN * 2 * width,
            bytes_accessed=tokens * width * 12,
            transcendentals=tokens * 3 * MOST_LEN * width // HEAD_DIM,
        ),
        compiler_params=pltpu.CompilerParams(vmem_limit_bytes=48 << 20),
        name="attend",
    )(project, project, project, feature_q, feature_k)


def attention_backward(project, feature_q, feature_k, grad_mixed, totals):
    tokens, width = grad_mixed.shape
    pairs = width // PAIR
    ins, own = attention_specs(pairs)
    low = jax.ShapeDtypeStruct((tokens, width), bf16)
    return pl.pallas_call(
        attention_backward_kernel,
        grid=(tokens // SEQ, pairs),
        in_specs=ins + [own, own],
        out_specs=[own, own, own, pl.BlockSpec((1, 8, PAIR), lambda r, p: (r, 0, p))],
        out_shape=[low, low, low, jax.ShapeDtypeStruct((tokens // SEQ, 8, width), f32)],
        scratch_shapes=[pltpu.VMEM((SEQ, PAIR), f32), pltpu.VMEM((SEQ, PAIR), f32)],
        cost_estimate=pl.CostEstimate(
            flops=10 * tokens * 3 * MOST_LEN * 2 * width,
            bytes_accessed=tokens * width * 18,
            transcendentals=tokens * 3 * MOST_LEN * width // HEAD_DIM,
        ),
        compiler_params=pltpu.CompilerParams(vmem_limit_bytes=48 << 20),
        name="attend_back",
    )(project, project, project, feature_q, feature_k, grad_mixed, totals)


def unpack_kernel(got_ref, qkv_ref, up_ref, down_ref, out_ref):
    blocks, hidden, few = up_ref.shape[1], up_ref.shape[2], out_ref.shape[2]
    for block in range(blocks):
        up_ref[0, block] = got_ref[block, 0, :hidden, :]
        down_ref[0, block] = got_ref[block, 0, hidden : 2 * hidden, :]
        out_ref[0, block] = got_ref[block, 0, 2 * hidden : 2 * hidden + few, :]
        for part in range(3):
            first = 2 * hidden + (1 + part) * few
            qkv_ref[part, 0, block] = got_ref[block, 0, first : first + few, :]


def unpack(got, hidden, few):
    n_dp, n_tensor, rows, width = got.shape

    def spec(count):
        return pl.BlockSpec((1, n_dp, count, width), lambda t: (t, 0, 0, 0))

    def shape(count):
        return jax.ShapeDtypeStruct((n_tensor, n_dp, count, width), bf16)

    outs = pl.pallas_call(
        unpack_kernel,
        grid=(n_tensor,),
        in_specs=[pl.BlockSpec((n_dp, 1, rows, width), lambda t: (0, t, 0, 0))],
        out_specs=[
            pl.BlockSpec((3, 1, n_dp, few, width), lambda t: (0, t, 0, 0, 0)),
            spec(hidden),
            spec(hidden),
            spec(few),
        ],
        out_shape=[
            jax.ShapeDtypeStruct((3, n_tensor, n_dp, few, width), bf16),
            shape(hidden),
            shape(hidden),
            shape(few),
        ],
        cost_estimate=pl.CostEstimate(
            flops=0, bytes_accessed=4 * n_dp * n_tensor * rows * width, transcendentals=0
        ),
        compiler_params=pltpu.CompilerParams(vmem_limit_bytes=48 << 20),
        name="unpack",
    )(got)
    return [array.reshape(-1, width) for array in outs]


class PermuteSum:
    def __init__(self, blocks):
        sizes = {axis: lax.axis_size(axis) for axis in groups}
        self.blocks = blocks
        self.steps = [
            (axis, bit) for axis in groups for bit in range(sizes[axis].bit_length() - 1)
        ]

    def step(self):
        axis, bit = self.steps.pop(0)
        pairs = [(index, index ^ (1 << bit)) for index in range(lax.axis_size(axis))]
        self.blocks = self.blocks + lax.ppermute(self.blocks, axis, pairs)


class PermuteScatter:
    def __init__(self, blocks, order):
        self.bits = {axis: lax.axis_size(axis).bit_length() - 1 for axis in groups}
        self.left = [(axis, bit) for axis in groups for bit in reversed(range(self.bits[axis]))]
        self.blocks = blocks.reshape((2,) * len(self.left) + blocks.shape[2:])
        self.steps = order(self.bits)

    def step(self):
        axis, bit = self.steps.pop(0)
        dim = self.left.index((axis, bit))
        self.left.pop(dim)
        side = (lax.axis_index(axis) >> bit) & 1
        sent = lax.dynamic_index_in_dim(self.blocks, 1 - side, dim, keepdims=False)
        own = lax.dynamic_index_in_dim(self.blocks, side, dim, keepdims=False)
        pairs = [(index, index ^ (1 << bit)) for index in range(1 << self.bits[axis])]
        blocks = own.astype(f32) + lax.ppermute(sent, axis, pairs).astype(f32)
        self.blocks = blocks.astype(bf16) if self.left else blocks


def tie(value, chains):
    value, blocks = lax.optimization_barrier((value, [chain.blocks for chain in chains]))
    for chain, block in zip(chains, blocks):
        chain.blocks = block
    return value


def advance(value, chains):
    chains = [chain for chain in chains if chain.steps]
    for chain in chains:
        chain.step()
    return tie(value, chains)


def rising(bits):
    return [(axis, bit) for axis in groups for bit in range(bits[axis])]


def turned_about(bits):
    steps = rising(bits)
    count = bits[groups[0]]
    return steps[:1] + steps[1:count][::-1] + steps[count:]


def wide_kernel(norm_ref, up_ref, branch_ref, active_ref, out_ref, turned, result):
    piece = out_ref.shape[3]
    step = pl.program_id(0)
    for position, (left_ref, right_ref) in enumerate(
        ((norm_ref, up_ref), (branch_ref, active_ref))
    ):

        @pl.when(step == position)
        def _():
            @pl.when(pl.program_id(1) == 0)
            def _():
                turned[...] = left_ref[...].T

            result[...] = jnp.dot(turned[...], right_ref[...], preferred_element_type=f32)

    for block in range(out_ref.shape[0]):
        out_ref[block, 0, 0] = result[block * piece : (block + 1) * piece, :].astype(bf16)


def narrow_kernel(
    norm_ref, dq_ref, dk_ref, dv_ref, branch_ref, mixed_ref,
    out_ref, turned, result,
):
    blocks, shards, _, piece, columns = out_ref.shape
    columns //= 4
    for position, right_ref in enumerate((dq_ref, dk_ref, dv_ref, mixed_ref)):
        if position == 0:
            turned[...] = norm_ref[...].T
        if position == 3:
            turned[...] = branch_ref[...].T
        result[...] = jnp.dot(turned[...], right_ref[...], preferred_element_type=f32)
        for block in range(blocks):
            for shard in range(shards):
                out_ref[block, shard, 0, :, position * columns : (position + 1) * columns] = (
                    result[
                        block * piece : (block + 1) * piece,
                        shard * columns : (shard + 1) * columns,
                    ].astype(bf16)
                )


def blocked_gradients(kernel, ins, in_specs, grid, out_spec, shape, products, name):
    tokens, width = ins[0].shape
    return pl.pallas_call(
        kernel,
        grid=grid,
        in_specs=in_specs,
        out_specs=out_spec,
        out_shape=[jax.ShapeDtypeStruct(shape, bf16)] * len(out_spec),
        scratch_shapes=[pltpu.VMEM((width, tokens), bf16), pltpu.VMEM((width, width), f32)],
        cost_estimate=pl.CostEstimate(
            flops=2 * products * tokens * width * width,
            bytes_accessed=products * 2 * (tokens * width + width * width),
            transcendentals=0,
        ),
        compiler_params=pltpu.CompilerParams(vmem_limit_bytes=56 << 20),
        name=name,
    )(*ins)


def wide_gradients(normed, grad_up, branch, active, shape):
    tokens, width = normed.shape
    n_dp, n_tensor, _, piece, _ = shape
    whole = pl.BlockSpec((tokens, width), lambda s, t: (0, 0))
    last = n_tensor - 1
    return blocked_gradients(
        wide_kernel,
        [normed, grad_up, branch, active],
        [
            whole,
            pl.BlockSpec((tokens, width), lambda s, t: (0, jnp.where(s == 0, t, last))),
            whole,
            pl.BlockSpec((tokens, width), lambda s, t: (0, jnp.where(s == 1, t, 0))),
        ],
        (2, n_tensor),
        [pl.BlockSpec((n_dp, 1, 1, piece, width), lambda s, t: (0, t, s, 0, 0))],
        shape,
        2 * n_tensor,
        "wide_grads",
    )


def narrow_gradients(normed, grads, branch, mixed, shape):
    tokens, width = normed.shape
    n_dp, n_tensor, _, piece, _ = shape
    whole = pl.BlockSpec((tokens, width), lambda s: (0, 0))
    return blocked_gradients(
        narrow_kernel,
        [normed, *grads, branch, mixed],
        [whole] * 6,
        (1,),
        [pl.BlockSpec((n_dp, n_tensor, 1, piece, width), lambda s: (0, 0, 0, 0, 0))],
        shape,
        4,
        "narrow_grads",
    )


def per_device(
    tokens,
    cotangent,
    lengths,
    drop_mask,
    ln1_gain,
    ln1_bias,
    w_qkv,
    b_qv,
    w_out,
    b_out,
    ln2_gain,
    ln2_bias,
    w_up,
    b_up,
    w_down,
    b_down,
):
    layer_count = w_qkv.shape[0]
    local_rows, width = tokens.shape
    segment_count = lengths.shape[1]
    tensor_index = lax.axis_index("tensor")
    dp_index = lax.axis_index("dp")
    n_dp = lax.axis_size("dp")
    n_tensor = lax.axis_size("tensor")
    own_rows = local_rows // SEQ
    head_cols = w_qkv.shape[3]
    hidden_cols = w_up.shape[2]
    piece = width // n_dp
    out_piece = head_cols // n_dp
    hidden_piece = hidden_cols // n_dp

    own_lengths = lax.dynamic_slice_in_dim(lengths, tensor_index * own_rows, own_rows, 0)
    own_mask = lax.dynamic_slice_in_dim(drop_mask, tensor_index * own_rows, own_rows, 2)
    segment_ends = jnp.cumsum(own_lengths, axis=-1)
    positions = jnp.arange(SEQ, dtype=jnp.int32)
    segments = jnp.sum(
        (positions[None, :, None] >= segment_ends[:, None, :]).astype(jnp.int32), axis=-1
    )
    onehot = (
        segments[:, :, None] == jnp.arange(segment_count, dtype=jnp.int32)[None, None, :]
    ).astype(f32)
    keep = (
        jnp.sum(onehot[None, None] * own_mask.astype(f32)[:, :, :, None, :], axis=-1) / survival
    ).reshape(layer_count, 2, local_rows)
    lane = jnp.arange(PAIR, dtype=jnp.int32)[None, :] % HEAD_DIM
    same = segments.reshape(local_rows, 1) == lane
    feature_q = same.astype(bf16)
    feature_k = jnp.where(same | (lane >= segment_count), 0.0, masked_score).astype(bf16)

    def gather(pieces):
        rows = jnp.concatenate(pieces, axis=0)
        gathered = lax.all_gather(rows, groups, axis=0, tiled=False)
        return gathered.reshape((n_dp, n_tensor) + rows.shape)

    def part_of(array, size, axis):
        return lax.dynamic_slice_in_dim(array, dp_index * size, size, axis)

    def qkv_piece(layer):
        turned = w_qkv[layer].transpose(1, 2, 0)
        return part_of(turned, out_piece, 1).reshape(3 * out_piece, width)

    def pieces_of(layer):
        return [
            part_of(w_up[layer], hidden_piece, 1).T,
            part_of(w_down[layer], hidden_piece, 0),
            part_of(w_out[layer], out_piece, 0),
            qkv_piece(layer),
        ]

    def rows_of(got, first, count, parts=1):
        rows = got[:, :, first : first + parts * count]
        rows = rows.reshape(n_dp, n_tensor, parts, count, width).transpose(2, 1, 0, 3, 4)
        return lax.optimization_barrier(rows.reshape(parts * n_dp * n_tensor * count, width))

    def weights_of(got):
        if piece % 16 == 0 and hidden_piece == piece and out_piece % 8 == 0:
            return unpack(got, hidden_piece, out_piece)
        up = rows_of(got, 0, hidden_piece)
        down = rows_of(got, hidden_piece, hidden_piece)
        out = rows_of(got, 2 * hidden_piece, out_piece)
        return rows_of(got, 2 * hidden_piece + out_piece, out_piece, 3), up, down, out

    weight_rows = 2 * hidden_piece + 4 * out_piece
    bias_rows = jnp.concatenate([b_qv.reshape(-1), b_up.reshape(-1)])
    bias_rows = jnp.pad(bias_rows, (0, 8 * width - bias_rows.shape[0])).reshape(8, width)
    full = []
    hidden = tokens.astype(f32)
    early = (norm_forward(hidden, ln1_gain[0], ln1_bias[0]), feature_q, feature_k, keep)
    for layer in range(layer_count):
        pieces = pieces_of(layer)
        if layer == 0:
            got = gather(pieces + [bias_rows])
            all_bias = got[0, :, weight_rows:].reshape(n_tensor, 8 * width).astype(f32)
        else:
            pieces, got, early = lax.optimization_barrier((pieces, got, early))
            full.append(weights_of(got))
            got = gather(pieces)
    full.append(weights_of(got))

    qv_count = layer_count * 2 * head_cols
    bias_qv = (
        all_bias[:, :qv_count]
        .reshape(n_tensor, layer_count, 2, head_cols)
        .transpose(1, 2, 0, 3)
        .reshape(layer_count, 2, width)
    )
    bias_up = (
        all_bias[:, qv_count : qv_count + layer_count * hidden_cols]
        .reshape(n_tensor, layer_count, hidden_cols)
        .transpose(1, 0, 2)
        .reshape(layer_count, n_tensor * hidden_cols)
    )

    first_norm, feature_q, feature_k, keep = early
    produced = []
    kept = []
    for layer in range(layer_count):
        if layer > 0:
            first_norm = norm_forward(hidden, ln1_gain[layer], ln1_bias[layer])
        normed_one, unit_one, scaled_one = first_norm
        normed_one = normed_one.astype(bf16)
        bias = jnp.concatenate([bias_qv[layer, 0], jnp.zeros((width,), f32), bias_qv[layer, 1]])
        full_qkv, full_up, full_down, full_out = full[layer]
        project = (dot_rows(normed_one, full_qkv) + bias).astype(bf16)
        mixed, totals = attention_forward(project, feature_q, feature_k)
        attn = jnp.dot(mixed, full_out, preferred_element_type=f32)
        middle = hidden + keep[layer, 0][:, None] * (attn + b_out[layer].astype(f32))
        normed_two, unit_two, scaled_two = norm_forward(middle, ln2_gain[layer], ln2_bias[layer])
        normed_two = normed_two.astype(bf16)
        upward = dot_rows(normed_two, full_up) + bias_up[layer]
        phi = 0.5 * (1.0 + lax.erf(upward * math.sqrt(0.5)))
        active = (upward * phi).astype(bf16)
        slope = phi + upward * (jnp.exp(-0.5 * upward * upward) * (1.0 / math.sqrt(2 * math.pi)))
        down = jnp.dot(active, full_down, preferred_element_type=f32)
        hidden = middle + keep[layer, 1][:, None] * (down + b_down[layer].astype(f32))
        produced.append(hidden.astype(bf16))
        kept.append(
            (unit_one, scaled_one, normed_one, project, totals, mixed,
             unit_two, scaled_two, normed_two, active, slope)
        )
    blocks_out = jnp.stack(produced)

    def scatter(blocks):
        flat = blocks.reshape((-1,) + blocks.shape[3:])
        flat = flat.reshape(-1, width)
        summed = lax.psum_scatter(flat, groups, scatter_dimension=0, tiled=True)
        return summed.reshape(blocks.shape[2:]).astype(f32)

    grad_flow = cotangent.astype(f32)
    collected = [None] * layer_count
    wide_sums = [None] * layer_count
    narrow_sums = [None] * layer_count
    chains = []
    paired = all(lax.axis_size(axis) & (lax.axis_size(axis) - 1) == 0 for axis in groups)
    for layer in reversed(range(layer_count)):
        (unit_one, scaled_one, normed_one, project, totals, mixed,
         unit_two, scaled_two, normed_two, active, slope) = kept[layer]
        full_qkv, full_up, full_down, full_out = full[layer]
        grad_flow = advance(grad_flow, chains)
        branch_two = keep[layer, 1][:, None] * grad_flow
        grad_bias_down = jnp.sum(branch_two, axis=0)
        branch_two = branch_two.astype(bf16)
        grad_up = dot_rows(branch_two, full_down) * slope
        grad_bias_up = jnp.sum(grad_up, axis=0)
        grad_up = grad_up.astype(bf16)
        wide = (normed_two, grad_up, branch_two, active)
        (wide,) = wide_gradients(*wide, (n_dp, n_tensor, 2, piece, width))
        grad_up, wide = lax.optimization_barrier((grad_up, wide))
        grad_up = advance(grad_up, chains)
        wide_sums[layer] = scatter(wide)
        grad_part, grad_gain_two, grad_shift_two = norm_backward(
            jnp.dot(grad_up, full_up, preferred_element_type=f32),
            unit_two, scaled_two, ln2_gain[layer],
        )
        grad_middle = grad_flow + grad_part
        branch_one = keep[layer, 0][:, None] * grad_middle
        grad_bias_out = jnp.sum(branch_one, axis=0)
        branch_one = branch_one.astype(bf16)
        grad_mixed = dot_rows(branch_one, full_out).astype(bf16)
        grad_mixed = advance(grad_mixed, chains)
        *grads, sums = attention_backward(project, feature_q, feature_k, grad_mixed, totals)
        grad_bias_qv = jnp.sum(sums, axis=0)[:2]
        if layer == 0:
            wide_sums[-1], *grads = lax.optimization_barrier((wide_sums[-1], *grads))
        grads = advance(grads, chains)
        (narrow,) = narrow_gradients(
            normed_one, grads, branch_one, mixed, (n_dp, n_tensor, 1, piece, width)
        )
        grads, narrow = lax.optimization_barrier((grads, narrow))
        if not paired:
            narrow_sums[layer] = [scatter(narrow)[0]]
        elif layer == 0 and piece % 2 == 0:
            narrow_sums[layer] = [
                PermuteScatter(part, order)
                for part, order in zip(
                    jnp.split(narrow[:, :, 0], 2, axis=2), (rising, turned_about)
                )
            ]
        else:
            narrow_sums[layer] = [PermuteScatter(narrow[:, :, 0], rising)]
        if paired:
            chains = chains + narrow_sums[layer]
        grad_one = sum(
            jnp.dot(
                grads[part],
                full_qkv[part * width : (part + 1) * width],
                preferred_element_type=f32,
            )
            for part in range(3)
        )
        grad_part, grad_gain_one, grad_shift_one = norm_backward(
            grad_one, unit_one, scaled_one, ln1_gain[layer]
        )
        grad_flow = grad_middle + grad_part
        collected[layer] = [
            grad_gain_one, grad_shift_one, grad_bias_qv[0], grad_bias_qv[1], grad_bias_out,
            grad_gain_two, grad_shift_two, grad_bias_down,
            *grad_bias_up.reshape(-1, width),
        ]
    small = jnp.stack([row for rows in collected for row in rows])
    if paired:
        small = PermuteSum(advance(small, chains))
        chains = chains + [small]
        while any(chain.steps for chain in chains):
            advance((), chains)
        small = small.blocks
    else:
        small = lax.psum(small, groups)
    grad_qkv, grad_out, grad_up, grad_down = [], [], [], []
    for layer in range(layer_count):
        narrow, wide = [
            [part.blocks if isinstance(part, PermuteScatter) else part for part in sums[layer]]
            for sums in (narrow_sums, wide_sums)
        ]
        narrow = jnp.concatenate(narrow, axis=0)
        grad_qkv.append(narrow[:, : 3 * head_cols].reshape(piece, 3, head_cols))
        grad_out.append(narrow[:, 3 * head_cols :].T)
        grad_up.append(wide[0])
        grad_down.append(wide[1].T)
    grad_qkv, grad_out, grad_up, grad_down = [
        jnp.stack(parts) for parts in (grad_qkv, grad_out, grad_up, grad_down)
    ]
    small = small.reshape(layer_count, -1)
    gain_one, shift_one, query_bias, value_bias, bias_out, gain_two, shift_two, bias_down = [
        small[:, position * width : (position + 1) * width] for position in range(8)
    ]
    return (
        blocks_out,
        grad_flow,
        gain_one,
        shift_one,
        grad_qkv,
        jnp.stack([query_bias, value_bias], axis=1),
        grad_out,
        bias_out,
        gain_two,
        shift_two,
        grad_up,
        small[:, 8 * width :],
        grad_down,
        bias_down,
    )


def solution(mesh):
    in_specs = (
        P(("dp", "tensor"), None),
        P(("dp", "tensor"), None),
        P("dp", None),
        P(None, None, "dp", None),
        P(),
        P(),
        P(None, None, None, "tensor"),
        P(None, None, "tensor"),
        P(None, "tensor", None),
        P(),
        P(),
        P(),
        P(None, None, "tensor"),
        P(None, "tensor"),
        P(None, "tensor", None),
        P(),
    )
    out_specs = (
        P(None, ("dp", "tensor"), None),
        P(("dp", "tensor"), None),
        P(),
        P(),
        P(None, "dp", None, "tensor"),
        P(),
        P(None, "tensor", "dp"),
        P(),
        P(),
        P(),
        P(None, "dp", "tensor"),
        P(),
        P(None, "tensor", "dp"),
        P(),
    )
    return jax.shard_map(
        per_device, mesh=mesh, in_specs=in_specs, out_specs=out_specs, check_vma=False
    )
```
